256 devices in a mesh: gx: 8 (over z_hi, y), gy: 8 (over z_lo, core), gz: 4 (over x).
Axes of the slice: x: 4, y: 4, z: 8 (z_hi: 2, z_lo: 4; z = z_hi * 4 + z_lo), core: 2. Of those that a mesh axis runs over, the one named last changes fastest.
Arguments:
- concentration: float32 [128, 512, 512], P('gx', 'gy', 'gz'), may hold values from -6 to 6
- speed: float32 [3, 128, 512, 512], P(None, 'gx', 'gy', 'gz'), may hold values from 0.1 to 1
- signs: int32 [3, 128, 512, 512], P(None, 'gx', 'gy', 'gz'), may hold values from 0 to 1
- diffusivity: float32 [128, 512, 512], P('gx', 'gy', 'gz'), may hold values from 0.02 to 0.12
- shear: int32 [1], replicated, may hold values from 0 to 511
Outputs:
- final_field: float32 [128, 512, 512], P('gx', 'gy', 'gz')
The draws below stay inside these ranges and needn't reach their ends.
All inputs are finite; a program needn't handle non-finite values.
Results may differ from the reference program's by a relative error of at most 0.00002.
Values sent between devices are 32-bit elements; how exact they have to be, the bound alone decides.
No kernel may reach another device: no remote copies, remote signals or barrier semaphores. Data moves between devices by JAX's collectives and lax.ppermute only.
A program may use at most 64 MiB of HBM per device.

```python
import math
import jax
import jax.numpy as jnp

STEPS = 8
NX = 128
NY = 512
NZ = 512


def with_ends(values, rng, low, largest):
    shape = values.shape
    place = [jax.random.randint(jax.random.fold_in(rng, axis), (), 0, shape[axis]) for axis in range(len(shape))]
    values = values.at[tuple(place)].set(low)
    longest = shape.index(max(shape))
    place[longest] = (place[longest] + 1) % shape[longest]
    return values.at[tuple(place)].set(largest)


def level_of(rng, shape, shards, least, high):
    loudness, own = 1.0, jax.random.fold_in(rng, 6)
    for position, parts in shards:
        draws = jnp.exp(jax.random.uniform(jax.random.fold_in(own, position), (parts,), jnp.float32, least / len(shards), high / len(shards)))
        loudness = loudness * jnp.repeat(draws, shape[position] // parts).reshape([-1 if axis == position else 1 for axis in range(len(shape))])
    return loudness


def scatter_about(own_key, dims, width, limit, pieces=(), kind=jnp.bfloat16):
    entries = width * jax.random.normal(own_key, dims, jnp.float32)
    if pieces:
        entries = entries * level_of(own_key, dims, pieces, -0.22, 0.18)
    return jnp.clip(entries, -limit, limit).astype(kind)


def setup_inputs(seed: int = 0) -> dict:
    key_list = jax.random.split(jax.random.key(seed), 6)
    concentration = scatter_about(key_list[0], (NX, NY, NZ), 1.0, 6.0, ((0, 8), (1, 8), (2, 4)), jnp.float32)
    speed = jnp.clip(jnp.exp(math.log(1.0) - 2.3025851 * jax.random.uniform(key_list[1], (3, NX, NY, NZ), jnp.float32) ** level_of(key_list[1], (3, NX, NY, NZ), ((1, 8), (2, 8), (3, 4)), -0.2, 0.2)), 0.1, 1.0)
    signs = with_ends(jax.random.randint(key_list[2], (3, NX, NY, NZ), 0, 2), jax.random.fold_in(key_list[2], 1), 0, 1).astype(jnp.int32)
    diffusivity = jnp.clip(jnp.exp(math.log(0.12) - 1.7917595 * jax.random.uniform(key_list[3], (NX, NY, NZ), jnp.float32) ** level_of(key_list[3], (NX, NY, NZ), ((0, 8), (1, 8), (2, 4)), -0.2, 0.2)), 0.02, 0.12)
    shear = jax.random.randint(key_list[4], (1,), 0, NY).astype(jnp.int32)
    return {"concentration": concentration, "speed": speed, "signs": signs, "diffusivity": diffusivity, "shear": shear}


time_step = 0.25


def advance(field, neighbours, speed, signs, diffusivity):
    total = jnp.zeros_like(field)
    for axis_id in range(3):
        below, above = neighbours[axis_id]
        upwind = jnp.where(signs[axis_id] > 0, field - below, above - field)
        total = total + diffusivity * (above + below - 2.0 * field) - speed[axis_id] * upwind
    return field + time_step * total


def reference(concentration, speed, signs, diffusivity, shear):
    offset = shear[0]
    field = concentration
    for step in range(STEPS):
        lower = jnp.roll(field[-1], -offset, axis=0)
        upper = jnp.roll(field[0], offset, axis=0)
        x_minus = jnp.concatenate([lower[None], field[:-1]], axis=0)
        x_plus = jnp.concatenate([field[1:], upper[None]], axis=0)
        y_minus = jnp.roll(field, 1, axis=1)
        y_plus = jnp.roll(field, -1, axis=1)
        z_minus = jnp.roll(field, 1, axis=2)
        z_plus = jnp.roll(field, -1, axis=2)
        field = advance(field, ((x_minus, x_plus), (y_minus, y_plus), (z_minus, z_plus)), speed, signs, diffusivity)
    return field
```

```python
import functools

import jax
import jax.numpy as jnp
from jax import lax
from jax.experimental import pallas as pl
from jax.experimental.pallas import tpu as pltpu
from jax.sharding import PartitionSpec as P

STEPS = 8
WIDTH = 4
TIME_STEP = 0.25
PAD = 16
EDGE = 8
LANES = 128

VMEM = pl.BlockSpec(memory_space=pltpu.VMEM)
SMEM = pl.BlockSpec(memory_space=pltpu.SMEM)
DEPTHS = (WIDTH, WIDTH - 1, WIDTH - 1, WIDTH - 1, WIDTH - 1)


def call(kernel, outs, args, scratch=(), scalars=0):
    return pl.pallas_call(
        kernel,
        out_shape=[jax.ShapeDtypeStruct(shape, jnp.float32) for shape in outs],
        in_specs=[SMEM] * scalars + [VMEM] * (len(args) - scalars),
        out_specs=[VMEM] * len(outs),
        scratch_shapes=[pltpu.VMEM(shape, jnp.float32) for shape in scratch],
    )(*args)


def prepare(odd_ref, field, speed, signs, diffusivity, own, to_odd, to_even):
    nx = field.shape[0]

    def plane(x, carry):
        own[x] = field[x]
        own[nx + x] = TIME_STEP * diffusivity[x]
        for d in range(3):
            scaled = TIME_STEP * speed[d, x]
            own[(2 + d) * nx + x] = jnp.where(signs[d, x] > 0, scaled, -scaled)
        return carry

    lax.fori_loop(0, nx, plane, 0)
    faces(odd_ref[0], own, to_odd, to_even, nx, DEPTHS)


def faces(odd, own, to_odd, to_even, nx, depths):
    at = 0
    for q, depth in enumerate(depths):
        last = q * nx + nx - depth
        first = q * nx
        a = jnp.where(odd > 0, last, first)
        b = jnp.where(odd > 0, first, last)
        for i in range(depth):
            to_odd[at + i] = own[a + i]
            to_even[at + i] = own[b + i]
        at += depth


def pack_y(own, xlo, xhi, up, down):
    rows = own.shape[1]
    at = 0
    for src in (own, xlo, xhi):

        def plane(i, carry, src=src, at=at):
            up[at + i] = src[i, rows - WIDTH : rows, :]
            down[at + i] = src[i, 0:WIDTH, :]
            return carry

        lax.fori_loop(0, src.shape[0], plane, 0)
        at += src.shape[0]


def pack_z(own, xlo, xhi, ylo, yhi, up, down):
    rows = own.shape[1]
    per = LANES // WIDTH
    segments, at = [], 0
    for src in (own, xlo, xhi):
        start = 0
        while start < src.shape[0]:
            count = min(src.shape[0] - start, per - at % per)
            segments.append((src, start, at, count))
            start += count
            at += count
    group = lax.broadcasted_iota(jnp.int32, (rows, LANES), 1) // WIDTH
    small = lax.broadcasted_iota(jnp.int32, (WIDTH, LANES), 1) // WIDTH
    zero = jnp.zeros((rows, LANES), jnp.float32)
    little = jnp.zeros((WIDTH, LANES), jnp.float32)
    state = None
    for src, start, at, count in segments:
        tile = at // per
        if at % per == 0:
            state = (zero, zero, little, little, little, little)

        def plane(i, state, src=src, start=start, at=at):
            m = at % per + i
            high, low = WIDTH * m + WIDTH, WIDTH * m
            high = jnp.where(high >= LANES, 0, high)
            out = []
            for k, value in enumerate((src[start + i], ylo[at + i], yhi[at + i])):
                mask = (group if k == 0 else small) == m
                out.append(jnp.where(mask, pltpu.roll(value, high, 1), state[2 * k]))
                out.append(jnp.where(mask, pltpu.roll(value, low, 1), state[2 * k + 1]))
            return tuple(out)

        state = lax.fori_loop(0, count, plane, state)
        for ref, k in ((up, 0), (down, 1)):
            ref[tile, EDGE : EDGE + rows, :] = state[k]
            ref[tile, EDGE - WIDTH : EDGE, :] = state[2 + k]
            ref[tile, EDGE + rows : EDGE + rows + WIDTH, :] = state[4 + k]


def lay_out(put, own, first, halo, q, nx, depths, before):
    xlo, xhi = halo[:2]
    at = sum(depths[:q])
    depth = depths[q]
    total = sum(depths)

    def plane(i, carry):
        put(WIDTH + i, first + i, own, first + i)
        return carry

    lax.fori_loop(0, nx, plane, 0)
    for i in range(depth):
        put(WIDTH - depth + i, before + at + i, xlo, at + i)
        put(WIDTH + nx + i, before + total + at + i, xhi, at + i)


def writer(store, halo, rows):
    ylo, yhi, zlo, zhi = halo[2:]
    per = LANES // WIDTH
    left = lax.broadcasted_iota(jnp.int32, (rows + 2 * EDGE, LANES), 1) < LANES // 2

    def put(x, p, src, index):
        store(0, x, PAD, src[index])
        store(0, x, PAD - WIDTH, ylo[p])
        store(0, x, PAD + rows, yhi[p])
        tile, m = p // per, p % per
        shift = (LANES - WIDTH) - WIDTH * m
        wrapped = LANES - WIDTH * m
        wrapped = jnp.where(wrapped >= LANES, 0, wrapped)
        side = jnp.where(left, pltpu.roll(zhi[tile], wrapped, 1), pltpu.roll(zlo[tile], shift, 1))
        store(1, x, PAD - EDGE, side)

    return put


def advance(second, *refs):
    odd_ref, own = refs[0], refs[1]
    coef_halo = refs[2:8]
    refs = refs[8:]
    if second:
        field_own, field_halo = refs[0], refs[1:7]
        out = refs[7]
        refs = refs[8:]
        nx = field_own.shape[0]
    else:
        out, to_odd, to_even = refs[:3]
        refs = refs[3:]
        nx = out.shape[0]
    cells, raw, coef = refs
    rows = own.shape[1]
    high = rows + 2 * EDGE

    put = writer(lambda side, x, row, v: cells.__setitem__((0, side, x, pl.ds(row, v.shape[0])), v), field_halo if second else coef_halo, rows)
    if second:
        lay_out(put, field_own, 0, field_halo, 0, nx, (WIDTH,), nx)
    else:
        lay_out(put, own, 0, coef_halo, 0, nx, DEPTHS, 5 * nx)
    for q in range(1, 5):

        def store(side, x, row, v, q=q):
            raw[q - 1, side, x, pl.ds(row - (PAD - EDGE), v.shape[0])] = v

        lay_out(writer(store, coef_halo, rows), own, q * nx, coef_halo, q, nx, DEPTHS, 5 * nx)

    def derive(x, carry):
        for side in range(2):
            for row in range(0, high, 16):
                at = pl.ds(row, 16)
                d = raw[0, side, x, at]
                v = [raw[1 + k, side, x, at] for k in range(3)]
                coef[0, side, x, at] = 1.0 - 6.0 * d - (v[0] + v[1] + v[2])
                for k in range(3):
                    coef[1 + 2 * k, side, x, at] = d + jnp.maximum(v[k], 0.0)
                    coef[2 + 2 * k, side, x, at] = d + jnp.minimum(v[k], 0.0)
        return carry

    lax.fori_loop(1, nx + 2 * WIDTH - 1, derive, 0)

    lane = lax.broadcasted_iota(jnp.int32, (16, LANES), 1)
    start, end = lane == 0, lane == LANES - 1
    for step in range(1, WIDTH + 1):
        src, dst = (step - 1) % 2, step % 2
        last = step == WIDTH

        def plane(x, carry, src=src, dst=dst, last=last):
            for row in range(EDGE if last else 0, high - EDGE if last else high, 16):
                here = PAD - EDGE + row
                at = pl.ds(row, 16)
                mid = [cells[src, side, x, pl.ds(here, 16)] for side in range(2)]
                below = [pltpu.roll(m, 1, 1) for m in mid]
                above = [pltpu.roll(m, LANES - 1, 1) for m in mid]
                for side in range(1 if last else 2):
                    c = [coef[k, side, x, at] for k in range(7)]
                    new = c[0] * mid[side]
                    new += c[1] * cells[src, side, x - 1, pl.ds(here, 16)]
                    new += c[2] * cells[src, side, x + 1, pl.ds(here, 16)]
                    new += c[3] * cells[src, side, x, pl.ds(here - 1, 16)]
                    new += c[4] * cells[src, side, x, pl.ds(here + 1, 16)]
                    new += c[5] * jnp.where(start, below[1 - side], below[side])
                    new += c[6] * jnp.where(end, above[1 - side], above[side])
                    if last:
                        out[x - WIDTH, pl.ds(row - EDGE, 16)] = new
                    else:
                        cells[dst, side, x, pl.ds(here, 16)] = new
            return carry

        lax.fori_loop(step, nx + 2 * WIDTH - step, plane, 0)
    if not second:
        faces(odd_ref[0], out, to_odd, to_even, nx, (WIDTH,))


def slab_pairs(count_x, count_y, shift):
    even, odd, slid = [], [], []
    for j in range(count_y):
        for i in range(0, count_x, 2):
            a, b = i * count_y + j, (i + 1) * count_y + j
            even += [(a, b), (b, a)]
        for i in range(1, count_x - 1, 2):
            a, b = i * count_y + j, (i + 1) * count_y + j
            odd += [(a, b), (b, a)]
        for pairs, extra in ((odd, 0), (slid, 1)):
            top = (count_x - 1) * count_y + (j + shift + extra) % count_y
            pairs += [(j, top), (top, j)]
    return even, odd, slid


def exchange_x(to_odd, to_even, offset, rows):
    count_x, count_y = lax.axis_size("gx"), lax.axis_size("gy")
    x_index = lax.axis_index("gx")

    def branch(shift):
        even, odd, slid = slab_pairs(count_x, count_y, shift)

        def run(a, b):
            return (
                lax.ppermute(a, ("gx", "gy"), odd),
                lax.ppermute(a, ("gx", "gy"), slid),
                lax.ppermute(b, ("gx", "gy"), even),
            )

        return run

    one, two, three = lax.switch(offset // rows, [branch(k) for k in range(count_y)], to_odd, to_even)
    rest = offset % rows
    top = x_index == count_x - 1
    start = jnp.where(x_index == 0, rest, jnp.where(top, rows - rest, 0))
    both = jnp.concatenate([jnp.where(top, two, one), jnp.where(top, one, two)], axis=1)
    one = lax.dynamic_slice_in_dim(both, start, rows, 1)
    odd = x_index % 2 == 1
    return jnp.where(odd, three, one), jnp.where(odd, one, three)


def shift_both(axis, up, down):
    n = lax.axis_size(axis)
    forth = [(i, (i + 1) % n) for i in range(n)]
    return lax.ppermute(up, axis, forth), lax.ppermute(down, axis, [(b, a) for a, b in forth])


def gather_halo(own, to_odd, to_even, offset):
    planes, rows, _ = own.shape
    xlo, xhi = exchange_x(to_odd, to_even, offset, rows)
    total = planes + 2 * xlo.shape[0]
    shape = (total, WIDTH, LANES)
    up, down = call(pack_y, [shape] * 2, [own, xlo, xhi])
    ylo, yhi = shift_both("gy", up, down)
    tiles = -(-total * WIDTH // LANES)
    shape = (tiles, rows + 2 * EDGE, LANES)
    up, down = call(pack_z, [shape] * 2, [own, xlo, xhi, ylo, yhi])
    zlo, zhi = shift_both("gz", up, down)
    return [xlo, xhi, ylo, yhi, zlo, zhi]


def body(concentration, speed, signs, diffusivity, shear):
    nx, rows, lanes = concentration.shape
    offset = shear[0]
    odd = (lax.axis_index("gx") % 2).astype(jnp.int32).reshape(1)
    face = (sum(DEPTHS), rows, lanes)
    own, to_odd, to_even = call(
        prepare, [(5 * nx, rows, lanes), face, face], [odd, concentration, speed, signs, diffusivity], scalars=1
    )
    halo = gather_halo(own, to_odd, to_even, offset)
    high = rows + 2 * EDGE
    wide = nx + 2 * WIDTH
    scratch = [(2, 2, wide, rows + 2 * PAD, lanes), (4, 2, wide, high, lanes), (7, 2, wide, high, lanes)]
    face = (WIDTH, rows, lanes)
    field, to_odd, to_even = call(
        functools.partial(advance, False), [(nx, rows, lanes), face, face], [odd, own] + halo, scratch, 1
    )
    later = gather_halo(field, to_odd, to_even, offset)
    (field,) = call(functools.partial(advance, True), [(nx, rows, lanes)], [odd, own] + halo + [field] + later, scratch, 1)
    return field


def solution(mesh):
    placed = (
        P("gx", "gy", "gz"),
        P(None, "gx", "gy", "gz"),
        P(None, "gx", "gy", "gz"),
        P("gx", "gy", "gz"),
        P(),
    )
    return jax.shard_map(
        body, mesh=mesh, in_specs=placed, out_specs=P("gx", "gy", "gz"), check_vma=False
    )
```

```python
import functools
import math

import jax
import jax.numpy as jnp
from jax import lax
from jax.experimental import pallas as pl
from jax.experimental.pallas import tpu as pltpu
from jax.sharding import PartitionSpec as P

STEPS = 8
WIDTH = 4
TIME_STEP = 0.25
PAD = 16
EDGE = 8
LANES = 128

VMEM = pl.BlockSpec(memory_space=pltpu.VMEM)
SMEM = pl.BlockSpec(memory_space=pltpu.SMEM)
DEPTHS = (WIDTH, WIDTH - 1, WIDTH - 1, WIDTH - 1, WIDTH - 1)


def call(kernel, outs, args, scratch=(), scalars=0):
    need = sum(4 * math.prod(shape) for shape in list(outs) + list(scratch))
    need += sum(4 * math.prod(arg.shape) for arg in args[scalars:])
    return pl.pallas_call(
        kernel,
        out_shape=[jax.ShapeDtypeStruct(shape, jnp.float32) for shape in outs],
        in_specs=[SMEM] * scalars + [VMEM] * (len(args) - scalars),
        out_specs=[VMEM] * len(outs),
        scratch_shapes=[pltpu.VMEM(shape, jnp.float32) for shape in scratch],
        compiler_params=pltpu.CompilerParams(vmem_limit_bytes=need + 4 * 2**20),
    )(*args)


def prepare(odd_ref, field, speed, signs, diffusivity, own, to_odd, to_even):
    nx = field.shape[0]

    def plane(x, carry):
        own[x] = field[x]
        own[nx + x] = TIME_STEP * diffusivity[x]
        for d in range(3):
            scaled = TIME_STEP * speed[d, x]
            own[(2 + d) * nx + x] = jnp.where(signs[d, x] > 0, scaled, -scaled)
        return carry

    lax.fori_loop(0, nx, plane, 0)
    faces(odd_ref[0], own, to_odd, to_even, nx, DEPTHS)


def faces(odd, own, to_odd, to_even, nx, depths):
    at = 0
    for q, depth in enumerate(depths):
        last = q * nx + nx - depth
        first = q * nx
        a = jnp.where(odd > 0, last, first)
        b = jnp.where(odd > 0, first, last)
        for i in range(depth):
            to_odd[at + i] = own[a + i]
            to_even[at + i] = own[b + i]
        at += depth


def pack_y(place, own, one, two, three, xlo, xhi, up, down, joined):
    odd, start = place[0], place[1]
    rows = own.shape[1]
    first, second = place[2], place[3]
    for i in range(xlo.shape[0]):
        joined[i, pl.ds(first, rows), :] = one[i]
        joined[i, pl.ds(second, rows), :] = two[i]
    for i in range(xlo.shape[0]):
        slid = joined[i, pl.ds(start, rows), :]
        other = three[i]
        xlo[i] = jnp.where(odd > 0, other, slid)
        xhi[i] = jnp.where(odd > 0, slid, other)
    at = 0
    for src in (own, xlo, xhi):
        for i in range(src.shape[0]):
            up[at + i] = src[i, rows - WIDTH : rows, :]
            down[at + i] = src[i, 0:WIDTH, :]
        at += src.shape[0]


def planes_of(q, nx, depths, own, xlo, xhi):
    depth, at, total = depths[q], sum(depths[:q]), sum(depths)
    base = len(depths) * nx
    low = [(WIDTH - depth + i, xlo, at + i, base + at + i) for i in range(depth)]
    mid = [(WIDTH + i, own, q * nx + i, q * nx + i) for i in range(nx)]
    high = [(WIDTH + nx + i, xhi, at + i, base + total + at + i) for i in range(depth)]
    return low + mid + high


def pack_z(depths, own, xlo, xhi, ylo, yhi, up, down):
    rows = own.shape[1]
    nx = own.shape[0] // len(depths)
    for q in range(len(depths)):
        planes = planes_of(q, nx, depths, own, xlo, xhi)
        pieces = [(EDGE + r, 32, lambda p, r=r: p[1][p[2], r : r + 32]) for r in range(0, rows, 32)]
        pieces += [(EDGE - WIDTH, WIDTH, lambda p: ylo[p[3]]), (EDGE + rows, WIDTH, lambda p: yhi[p[3]])]
        for row, count, read in pieces:
            lane = lax.broadcasted_iota(jnp.int32, (count, LANES), 1)
            pair, lower = lane // (2 * WIDTH), lane % (2 * WIDTH) < WIDTH
            sums = [jnp.zeros((count, LANES), jnp.float32)] * 2
            for p in planes:
                m, k = p[0] // 2, p[0] % 2
                moved = pltpu.roll(read(p), (2 * WIDTH * m + WIDTH) % LANES, 1)
                sums[k] = jnp.where(pair == m, moved, sums[k])
            up[q, row : row + count] = jnp.where(lower, sums[0], pltpu.roll(sums[1], WIDTH, 1))
            down[q, row : row + count] = jnp.where(lower, pltpu.roll(sums[0], LANES - WIDTH, 1), sums[1])


def derive(read, write):
    d = read(1)
    v = [read(2 + k) for k in range(3)]
    write(0, 1.0 - 6.0 * d - (v[0] + v[1] + v[2]))
    for k in range(3):
        write(1 + 2 * k, d + jnp.maximum(v[k], 0.0))
        write(2 + 2 * k, d + jnp.minimum(v[k], 0.0))


def advance(second, *refs):
    odd_ref, own = refs[0], refs[1]
    halo = refs[2:8]
    refs = refs[8:]
    if second:
        field_own, field_halo, depths = refs[0], refs[1:7], (WIDTH,)
        out = refs[7]
        refs = refs[8:]
    else:
        field_own, field_halo, depths = own, halo, DEPTHS
        out, to_odd, to_even = refs[:3]
        refs = refs[3:]
    nx = out.shape[0]
    cells, coef, strip, strip_coef = refs
    rows = own.shape[1]
    high = rows + 2 * EDGE
    shift = PAD - EDGE

    for x, src, index, p in planes_of(0, nx, depths, field_own, *field_halo[:2]):
        cells[0, x, PAD : PAD + rows] = src[index]
        cells[0, x, PAD - WIDTH : PAD] = field_halo[2][p]
        cells[0, x, PAD + rows : PAD + rows + WIDTH] = field_halo[3][p]
    for side in range(2):
        strip[0, side, shift : shift + high] = field_halo[4 + side][0]

        def write(k, value, side=side):
            strip_coef[k, side] = value

        derive(lambda q, side=side: halo[4 + side][q], write)
    by_place = zip(*[planes_of(q, nx, DEPTHS, own, *halo[:2]) for q in range(1, 5)])
    for four in by_place:
        x = four[0][0]

        def at(row, count, x=x):
            def write(k, value):
                coef[k, x, row : row + count] = value

            return write

        for r in range(0, rows, 16):
            derive(lambda q, r=r, four=four: four[q - 1][1][four[q - 1][2], r : r + 16], at(EDGE + r, 16))
        derive(lambda q, four=four: halo[2][four[q - 1][3]], at(EDGE - WIDTH, WIDTH))
        derive(lambda q, four=four: halo[3][four[q - 1][3]], at(EDGE + rows, WIDTH))

    for step in range(1, WIDTH + 1):
        src, dst = (step - 1) % 2, step % 2
        last = step == WIDTH
        size = rows // 2 if last else high // 2
        for row in (EDGE, EDGE + size) if last else (0, size):
            here = shift + row
            lane = lax.broadcasted_iota(jnp.int32, (size, LANES), 1)
            start, end = lane == 0, lane == LANES - 1
            group, place = lane // WIDTH, lane % WIDTH
            low, top = (strip[src, side, here : here + size] for side in range(2))
            beyond = jnp.where(place == WIDTH - 1, low, pltpu.roll(top, WIDTH - 2, 1))
            inner = jnp.zeros((size, LANES), jnp.float32)
            before = cells[src, step - 1, here : here + size]
            mid = cells[src, step, here : here + size]
            for x in range(step, nx + 2 * WIDTH - step):
                after = cells[src, x + 1, here : here + size]
                turn = WIDTH * x + WIDTH - 1
                outer = pltpu.roll(beyond, (LANES - turn) % LANES, 1)
                if not last:
                    inner = jnp.where(group == x, pltpu.roll(mid, turn % LANES, 1), inner)
                c = [coef[k, x, row : row + size] for k in range(7)]
                new = c[0] * mid + c[1] * before + c[2] * after
                new += c[3] * cells[src, x, here - 1 : here - 1 + size]
                new += c[4] * cells[src, x, here + 1 : here + 1 + size]
                new += c[5] * jnp.where(start, outer, pltpu.roll(mid, 1, 1))
                new += c[6] * jnp.where(end, outer, pltpu.roll(mid, LANES - 1, 1))
                if last:
                    out[x - WIDTH, row - EDGE : row - EDGE + size] = new
                else:
                    cells[dst, x, here : here + size] = new
                before, mid = mid, after
            if last:
                continue
            for side in range(2):
                mid = low if side == 0 else top
                below, above = pltpu.roll(mid, 1, 1), pltpu.roll(mid, LANES - 1, 1)
                if side == 0:
                    above = jnp.where(place == WIDTH - 1, inner, above)
                else:
                    below = jnp.where(place == 0, pltpu.roll(inner, LANES - (WIDTH - 2), 1), below)
                c = [strip_coef[k, side, row : row + size] for k in range(7)]
                new = c[0] * mid + c[1] * pltpu.roll(mid, WIDTH, 1) + c[2] * pltpu.roll(mid, LANES - WIDTH, 1)
                new += c[3] * strip[src, side, here - 1 : here - 1 + size]
                new += c[4] * strip[src, side, here + 1 : here + 1 + size]
                new += c[5] * below + c[6] * above
                strip[dst, side, here : here + size] = new
    if not second:
        faces(odd_ref[0], out, to_odd, to_even, nx, (WIDTH,))


def slab_pairs(count_x, count_y, shift):
    even, odd, slid = [], [], []
    for j in range(count_y):
        for i in range(0, count_x, 2):
            a, b = i * count_y + j, (i + 1) * count_y + j
            even += [(a, b), (b, a)]
        for i in range(1, count_x - 1, 2):
            a, b = i * count_y + j, (i + 1) * count_y + j
            odd += [(a, b), (b, a)]
        for pairs, extra in ((odd, 0), (slid, 1)):
            top = (count_x - 1) * count_y + (j + shift + extra) % count_y
            pairs += [(j, top), (top, j)]
    return even, odd, slid


def exchange_x(to_odd, to_even, offset, rows):
    count_x, count_y = lax.axis_size("gx"), lax.axis_size("gy")
    x_index = lax.axis_index("gx")

    def branch(shift):
        even, odd, slid = slab_pairs(count_x, count_y, shift)

        def run(a, b):
            return (
                lax.ppermute(a, ("gx", "gy"), odd),
                lax.ppermute(a, ("gx", "gy"), slid),
                lax.ppermute(b, ("gx", "gy"), even),
            )

        return run

    one, two, three = lax.switch(offset // rows, [branch(k) for k in range(count_y)], to_odd, to_even)
    rest = offset % rows
    top = x_index == count_x - 1
    start = jnp.where(x_index == 0, rest, jnp.where(top, rows - rest, 0))
    zero = jnp.where(top, rows, 0)
    place = jnp.stack([x_index % 2, start, zero, rows - zero]).astype(jnp.int32)
    return place, one, two, three


def shift_both(axis, up, down):
    n = lax.axis_size(axis)
    forth = [(i, (i + 1) % n) for i in range(n)]
    return lax.ppermute(up, axis, forth), lax.ppermute(down, axis, [(b, a) for a, b in forth])


def gather_halo(own, depths, to_odd, to_even, offset):
    planes, rows, _ = own.shape
    total = sum(depths)
    face = (total, rows, LANES)
    shape = (planes + 2 * total, WIDTH, LANES)
    args = [*exchange_x(to_odd, to_even, offset, rows)]
    args.insert(1, own)
    xlo, xhi, up, down = call(pack_y, [face, face, shape, shape], args, [(total, 2 * rows, LANES)], 1)
    ylo, yhi = shift_both("gy", up, down)
    shape = (len(depths), rows + 2 * EDGE, LANES)
    up, down = call(functools.partial(pack_z, depths), [shape] * 2, [own, xlo, xhi, ylo, yhi])
    zlo, zhi = shift_both("gz", up, down)
    return [xlo, xhi, ylo, yhi, zlo, zhi]


def body(concentration, speed, signs, diffusivity, shear):
    nx, rows, lanes = concentration.shape
    offset = shear[0]
    odd = (lax.axis_index("gx") % 2).astype(jnp.int32).reshape(1)
    face = (sum(DEPTHS), rows, lanes)
    own, to_odd, to_even = call(
        prepare, [(5 * nx, rows, lanes), face, face], [odd, concentration, speed, signs, diffusivity], scalars=1
    )
    halo = gather_halo(own, DEPTHS, to_odd, to_even, offset)
    high = rows + 2 * EDGE
    wide = nx + 2 * WIDTH
    scratch = [(2, wide, rows + 2 * PAD, lanes), (7, wide, high, lanes), (2, 2, rows + 2 * PAD, lanes), (7, 2, high, lanes)]
    face = (WIDTH, rows, lanes)
    field, to_odd, to_even = call(
        functools.partial(advance, False), [(nx, rows, lanes), face, face], [odd, own] + halo, scratch, 1
    )
    later = gather_halo(field, (WIDTH,), to_odd, to_even, offset)
    (field,) = call(functools.partial(advance, True), [(nx, rows, lanes)], [odd, own] + halo + [field] + later, scratch, 1)
    return field


def solution(mesh):
    placed = (
        P("gx", "gy", "gz"),
        P(None, "gx", "gy", "gz"),
        P(None, "gx", "gy", "gz"),
        P("gx", "gy", "gz"),
        P(),
    )
    return jax.shard_map(
        body, mesh=mesh, in_specs=placed, out_specs=P("gx", "gy", "gz"), check_vma=False
    )
```

```python
import functools
import math

import jax
import jax.numpy as jnp
from jax import lax
from jax.experimental import pallas as pl
from jax.experimental.pallas import tpu as pltpu
from jax.sharding import PartitionSpec as P

STEPS = 8
WIDTH = 4
TIME_STEP = 0.25
PAD = 16
EDGE = 8
LANES = 128

VMEM = pl.BlockSpec(memory_space=pltpu.VMEM)
SMEM = pl.BlockSpec(memory_space=pltpu.SMEM)
DEPTHS = (WIDTH, WIDTH - 1, WIDTH - 1, WIDTH - 1, WIDTH - 1)


def call(kernel, outs, args, scratch=(), scalars=0):
    need = sum(4 * math.prod(shape) for shape in list(outs) + list(scratch))
    need += sum(4 * math.prod(arg.shape) for arg in args[scalars:])
    return pl.pallas_call(
        kernel,
        out_shape=[jax.ShapeDtypeStruct(shape, jnp.float32) for shape in outs],
        in_specs=[SMEM] * scalars + [VMEM] * (len(args) - scalars),
        out_specs=[VMEM] * len(outs),
        scratch_shapes=[pltpu.VMEM(shape, jnp.float32) for shape in scratch],
        compiler_params=pltpu.CompilerParams(vmem_limit_bytes=need + 4 * 2**20),
    )(*args)


def prepare(odd_ref, field, speed, signs, diffusivity, own, to_odd, to_even):
    nx = field.shape[0]

    def plane(x, carry):
        own[x] = field[x]
        own[nx + x] = TIME_STEP * diffusivity[x]
        for d in range(3):
            scaled = TIME_STEP * speed[d, x]
            own[(2 + d) * nx + x] = jnp.where(signs[d, x] > 0, scaled, -scaled)
        return carry

    lax.fori_loop(0, nx, plane, 0)
    faces(odd_ref[0], own, to_odd, to_even, nx, DEPTHS)


def faces(odd, own, to_odd, to_even, nx, depths):
    at = 0
    for q, depth in enumerate(depths):
        last = q * nx + nx - depth
        first = q * nx
        a = jnp.where(odd > 0, last, first)
        b = jnp.where(odd > 0, first, last)
        for i in range(depth):
            to_odd[at + i] = own[a + i]
            to_even[at + i] = own[b + i]
        at += depth


def pack_y(place, own, one, slid, three, up, down, slid_up, slid_down):
    odd = place[0]
    rows = own.shape[1]
    total = one.shape[0]
    for i in range(own.shape[0]):
        up[i] = own[i, rows - WIDTH : rows, :]
        down[i] = own[i, 0:WIDTH, :]
    for src, base in ((one, odd), (three, 1 - odd)):
        for i in range(total):
            at = own.shape[0] + base * total + i
            up[at] = src[i, rows - WIDTH : rows, :]
            down[at] = src[i, 0:WIDTH, :]
    reach = slid_up.shape[1]
    for i in range(total):
        slid_up[i] = slid[i, rows - reach : rows, :]
        slid_down[i] = slid[i, 0:reach, :]


def planes_of(q, nx, depths, own, sides):
    depth, at, total = depths[q], sum(depths[:q]), sum(depths)
    low = [(WIDTH - depth + i, sides, at + i, None) for i in range(depth)]
    mid = [(WIDTH + i, own, q * nx + i, q * nx + i) for i in range(nx)]
    high = [(WIDTH + nx + i, sides, total + at + i, None) for i in range(depth)]
    return low + mid + high


def pack_z(depths, place, own, one, slid, three, ylo, yhi, slid_low, slid_high, sides, up, down, joined):
    rows = own.shape[1]
    nx = own.shape[0] // len(depths)
    total = one.shape[0]
    odd, crossed, start = place[0], place[1], place[2]
    high = rows + 2 * EDGE

    def framed(src, base, i):
        at = base * total + i
        sides[at, EDGE : EDGE + rows] = src[i]
        sides[at, EDGE - WIDTH : EDGE] = ylo[own.shape[0] + at]
        sides[at, EDGE + rows : EDGE + rows + WIDTH] = yhi[own.shape[0] + at]

    for i in range(total):
        framed(three, 1 - odd, i)

    @pl.when(crossed > 0)
    def _():
        reach = slid_low.shape[1]
        for i in range(total):
            joined[i, 0:reach] = slid_low[i]
            joined[i, reach : reach + rows] = slid[i]
            joined[i, reach + rows :] = slid_high[i]
        for i in range(total):
            sides[odd * total + i] = joined[i, pl.ds(start, high)]

    @pl.when(crossed == 0)
    def _():
        for i in range(total):
            framed(one, odd, i)

    for q in range(len(depths)):
        planes = planes_of(q, nx, depths, own, sides)
        for row, count in [(EDGE + r, 32) for r in range(0, rows, 32)] + [(EDGE - WIDTH, WIDTH), (EDGE + rows, WIDTH)]:
            lane = lax.broadcasted_iota(jnp.int32, (count, LANES), 1)
            pair, lower = lane // (2 * WIDTH), lane % (2 * WIDTH) < WIDTH
            sums = [jnp.zeros((count, LANES), jnp.float32)] * 2
            for x, src, index, p in planes:
                if p is None:
                    value = src[index, row : row + count]
                elif count == WIDTH:
                    value = (ylo if row < EDGE else yhi)[p]
                else:
                    value = src[index, row - EDGE : row - EDGE + count]
                m, k = x // 2, x % 2
                moved = pltpu.roll(value, (2 * WIDTH * m + WIDTH) % LANES, 1)
                sums[k] = jnp.where(pair == m, moved, sums[k])
            up[q, row : row + count] = jnp.where(lower, sums[0], pltpu.roll(sums[1], WIDTH, 1))
            down[q, row : row + count] = jnp.where(lower, pltpu.roll(sums[0], LANES - WIDTH, 1), sums[1])


def derive(read, write):
    d = read(1)
    v = [read(2 + k) for k in range(3)]
    write(0, 1.0 - 6.0 * d - (v[0] + v[1] + v[2]))
    for k in range(3):
        write(1 + 2 * k, d + jnp.maximum(v[k], 0.0))
        write(2 + 2 * k, d + jnp.minimum(v[k], 0.0))


def advance(second, *refs):
    odd_ref, own = refs[0], refs[1]
    halo = refs[2:7]
    refs = refs[7:]
    if second:
        field_own, field_halo, depths = refs[0], refs[1:6], (WIDTH,)
        out = refs[6]
        refs = refs[7:]
    else:
        field_own, field_halo, depths = own, halo, DEPTHS
        out, to_odd, to_even = refs[:3]
        refs = refs[3:]
    nx = out.shape[0]
    cells, coef, strip, strip_coef = refs
    rows = own.shape[1]
    high = rows + 2 * EDGE
    shift = PAD - EDGE

    for x, src, index, p in planes_of(0, nx, depths, field_own, field_halo[0]):
        if p is None:
            cells[0, x, shift : shift + high] = src[index]
            continue
        cells[0, x, PAD : PAD + rows] = src[index]
        cells[0, x, PAD - WIDTH : PAD] = field_halo[1][p]
        cells[0, x, PAD + rows : PAD + rows + WIDTH] = field_halo[2][p]
    for side in range(2):
        strip[0, side, shift : shift + high] = field_halo[3 + side][0]

        def write(k, value, side=side):
            strip_coef[k, side] = value

        derive(lambda q, side=side: halo[3 + side][q], write)
    for four in zip(*[planes_of(q, nx, DEPTHS, own, halo[0]) for q in range(1, 5)]):
        x, p = four[0][0], four[0][3]

        def at(row, count, x=x):
            def write(k, value):
                coef[k, x, row : row + count] = value

            return write

        offset = 0 if p is None else EDGE
        for r in range(0, high if p is None else rows, 16):
            derive(lambda q, r=r, four=four: four[q - 1][1][four[q - 1][2], r : r + 16], at(offset + r, 16))
        if p is not None:
            derive(lambda q, four=four: halo[1][four[q - 1][3]], at(EDGE - WIDTH, WIDTH))
            derive(lambda q, four=four: halo[2][four[q - 1][3]], at(EDGE + rows, WIDTH))

    for step in range(1, WIDTH + 1):
        src, dst = (step - 1) % 2, step % 2
        last = step == WIDTH
        size = rows // 2 if last else high // 2
        for row in (EDGE, EDGE + size) if last else (0, size):
            here = shift + row
            lane = lax.broadcasted_iota(jnp.int32, (size, LANES), 1)
            start, end = lane == 0, lane == LANES - 1
            group, place = lane // WIDTH, lane % WIDTH
            low, top = (strip[src, side, here : here + size] for side in range(2))
            beyond = jnp.where(place == WIDTH - 1, low, pltpu.roll(top, WIDTH - 2, 1))
            inner = jnp.zeros((size, LANES), jnp.float32)
            before = cells[src, step - 1, here : here + size]
            mid = cells[src, step, here : here + size]
            for x in range(step, nx + 2 * WIDTH - step):
                after = cells[src, x + 1, here : here + size]
                turn = WIDTH * x + WIDTH - 1
                outer = pltpu.roll(beyond, (LANES - turn) % LANES, 1)
                if not last:
                    inner = jnp.where(group == x, pltpu.roll(mid, turn % LANES, 1), inner)
                c = [coef[k, x, row : row + size] for k in range(7)]
                new = c[0] * mid + c[1] * before + c[2] * after
                new += c[3] * cells[src, x, here - 1 : here - 1 + size]
                new += c[4] * cells[src, x, here + 1 : here + 1 + size]
                new += c[5] * jnp.where(start, outer, pltpu.roll(mid, 1, 1))
                new += c[6] * jnp.where(end, outer, pltpu.roll(mid, LANES - 1, 1))
                if last:
                    out[x - WIDTH, row - EDGE : row - EDGE + size] = new
                else:
                    cells[dst, x, here : here + size] = new
                before, mid = mid, after
            if last:
                continue
            for side in range(2):
                mid = low if side == 0 else top
                below, above = pltpu.roll(mid, 1, 1), pltpu.roll(mid, LANES - 1, 1)
                if side == 0:
                    above = jnp.where(place == WIDTH - 1, inner, above)
                else:
                    below = jnp.where(place == 0, pltpu.roll(inner, LANES - (WIDTH - 2), 1), below)
                c = [strip_coef[k, side, row : row + size] for k in range(7)]
                new = c[0] * mid + c[1] * pltpu.roll(mid, WIDTH, 1) + c[2] * pltpu.roll(mid, LANES - WIDTH, 1)
                new += c[3] * strip[src, side, here - 1 : here - 1 + size]
                new += c[4] * strip[src, side, here + 1 : here + 1 + size]
                new += c[5] * below + c[6] * above
                strip[dst, side, here : here + size] = new
    if not second:
        faces(odd_ref[0], out, to_odd, to_even, nx, (WIDTH,))


def exchange_x(to_odd, to_even, shift):
    count_x, count_y = lax.axis_size("gx"), lax.axis_size("gy")
    even = [(i, i + 1) for i in range(0, count_x, 2)]
    odd = [(i, i + 1) for i in range(1, count_x - 1, 2)]

    def slide(k):
        pairs = []
        for j in range(count_y):
            top = (count_x - 1) * count_y + (j + k) % count_y
            pairs += [(j, top), (top, j)]
        return lambda a: lax.ppermute(a, ("gx", "gy"), pairs)

    three = lax.ppermute(to_even, "gx", even + [(b, a) for a, b in even])
    one = lax.ppermute(to_odd, "gx", odd + [(b, a) for a, b in odd])
    slid = lax.switch(shift, [slide(k) for k in range(count_y)], to_odd)
    return one, slid, three


def shift_both(axis, up, down):
    n = lax.axis_size(axis)
    forth = [(i, (i + 1) % n) for i in range(n)]
    return lax.ppermute(up, axis, forth), lax.ppermute(down, axis, [(b, a) for a, b in forth])


def gather_halo(own, depths, to_odd, to_even, shift, place):
    planes, rows, _ = own.shape
    total = sum(depths)
    count_x, count_y = lax.axis_size("gx"), lax.axis_size("gy")
    one, slid, three = exchange_x(to_odd, to_even, shift)
    shape = (planes + 2 * total, WIDTH, LANES)
    reach = rows // 2 + EDGE
    slid_shape = (total, reach, LANES)
    up, down, slid_up, slid_down = call(pack_y, [shape] * 2 + [slid_shape] * 2, [place, own, one, slid, three], (), 1)
    outer = [g * count_y + j for g in (0, count_x - 1) for j in range(count_y)]
    forth = [(i, i - i % count_y + (i + 1) % count_y) for i in outer]
    slid_low = lax.ppermute(slid_up, ("gx", "gy"), forth)
    slid_high = lax.ppermute(slid_down, ("gx", "gy"), [(b, a) for a, b in forth])
    ylo, yhi = shift_both("gy", up, down)
    high = rows + 2 * EDGE
    shape = (len(depths), high, LANES)
    sides, up, down = call(
        functools.partial(pack_z, depths),
        [(2 * total, high, LANES), shape, shape],
        [place, own, one, slid, three, ylo, yhi, slid_low, slid_high],
        [(total, rows + 2 * reach, LANES)],
        1,
    )
    zlo, zhi = shift_both("gz", up, down)
    return [sides, ylo, yhi, zlo, zhi]


def body(concentration, speed, signs, diffusivity, shear):
    nx, rows, lanes = concentration.shape
    count_x, count_y = lax.axis_size("gx"), lax.axis_size("gy")
    x_index = lax.axis_index("gx")
    blocks = (shear[0] + rows // 2) // rows
    shift, rest = blocks % count_y, shear[0] - blocks * rows
    crossed = (x_index == 0) | (x_index == count_x - 1)
    start = rows // 2 + jnp.where(x_index == 0, rest, -rest)
    odd = (x_index % 2).astype(jnp.int32).reshape(1)
    place = jnp.stack([x_index % 2, crossed.astype(jnp.int32), jnp.where(crossed, start, 0)]).astype(jnp.int32)
    face = (sum(DEPTHS), rows, lanes)
    own, to_odd, to_even = call(
        prepare, [(5 * nx, rows, lanes), face, face], [odd, concentration, speed, signs, diffusivity], scalars=1
    )
    halo = gather_halo(own, DEPTHS, to_odd, to_even, shift, place)
    high = rows + 2 * EDGE
    wide = nx + 2 * WIDTH
    scratch = [(2, wide, rows + 2 * PAD, lanes), (7, wide, high, lanes), (2, 2, rows + 2 * PAD, lanes), (7, 2, high, lanes)]
    face = (WIDTH, rows, lanes)
    field, to_odd, to_even = call(
        functools.partial(advance, False), [(nx, rows, lanes), face, face], [odd, own] + halo, scratch, 1
    )
    later = gather_halo(field, (WIDTH,), to_odd, to_even, shift, place)
    (field,) = call(functools.partial(advance, True), [(nx, rows, lanes)], [odd, own] + halo + [field] + later, scratch, 1)
    return field


def solution(mesh):
    placed = (
        P("gx", "gy", "gz"),
        P(None, "gx", "gy", "gz"),
        P(None, "gx", "gy", "gz"),
        P("gx", "gy", "gz"),
        P(),
    )
    return jax.shard_map(
        body, mesh=mesh, in_specs=placed, out_specs=P("gx", "gy", "gz"), check_vma=False
    )
```

```python
import functools
import math

import jax
import jax.numpy as jnp
from jax import lax
from jax.experimental import pallas as pl
from jax.experimental.pallas import tpu as pltpu
from jax.sharding import PartitionSpec as P

STEPS = 8
WIDTH = 4
TIME_STEP = 0.25
PAD = 16
EDGE = 8
LANES = 128

VMEM = pl.BlockSpec(memory_space=pltpu.VMEM)
SMEM = pl.BlockSpec(memory_space=pltpu.SMEM)
DEPTHS = (WIDTH, WIDTH - 1, WIDTH - 1, WIDTH - 1, WIDTH - 1)


def call(kernel, outs, args, scratch=(), scalars=0):
    need = sum(4 * math.prod(shape) for shape in list(outs) + list(scratch))
    need += sum(4 * math.prod(arg.shape) for arg in args[scalars:])
    return pl.pallas_call(
        kernel,
        out_shape=[jax.ShapeDtypeStruct(shape, jnp.float32) for shape in outs],
        in_specs=[SMEM] * scalars + [VMEM] * (len(args) - scalars),
        out_specs=[VMEM] * len(outs),
        scratch_shapes=[pltpu.VMEM(shape, jnp.float32) for shape in scratch],
        compiler_params=pltpu.CompilerParams(vmem_limit_bytes=need + 4 * 2**20),
    )(*args)


def first_faces(odd_ref, field, speed, signs, diffusivity, to_odd, to_even, f, s, g, d, sems):
    nx = field.shape[0]
    copies = []
    for side in range(2):
        deep, short = (pl.ds(nx - n if side else 0, n) for n in DEPTHS[:2])
        for src, dst in (
            (field.at[deep], f.at[side]),
            (diffusivity.at[short], d.at[side]),
            (speed.at[:, short], s.at[side]),
            (signs.at[:, short], g.at[side]),
        ):
            copies.append(pltpu.make_async_copy(src, dst, sems.at[len(copies)]))
    for copy in copies:
        copy.start()
    for copy in copies:
        copy.wait()
    odd = odd_ref[0]
    for out, side in ((to_odd, odd), (to_even, 1 - odd)):
        for i in range(WIDTH):
            out[i] = f[side, i]
        for i in range(WIDTH - 1):
            out[WIDTH + i] = TIME_STEP * d[side, i]
            for k in range(3):
                scaled = TIME_STEP * s[side, k, i]
                out[WIDTH + (1 + k) * (WIDTH - 1) + i] = jnp.where(g[side, k, i] > 0, scaled, -scaled)


def prepare(field, speed, signs, diffusivity, own, y_up, y_down, z_up, z_down):
    nx, rows = field.shape[:2]

    def plane(x, carry):
        own[x] = field[x]
        own[nx + x] = TIME_STEP * diffusivity[x]
        for d in range(3):
            scaled = TIME_STEP * speed[d, x]
            own[(2 + d) * nx + x] = jnp.where(signs[d, x] > 0, scaled, -scaled)
        return carry

    lax.fori_loop(0, nx, plane, 0)

    def edge(p, carry):
        y_up[p] = own[p, rows - WIDTH : rows, :]
        y_down[p] = own[p, 0:WIDTH, :]
        return carry

    lax.fori_loop(0, own.shape[0], edge, 0)

    def quantity(q, carry):
        for row in range(0, rows, 32):
            planes = [(WIDTH + i, own[q * nx + i, row : row + 32]) for i in range(nx)]
            up, down = pack_lanes(planes, 32)
            z_up[q, row : row + 32] = up
            z_down[q, row : row + 32] = down
        return carry

    lax.fori_loop(0, z_up.shape[0], quantity, 0)


def pack_lanes(planes, count):
    lane = lax.broadcasted_iota(jnp.int32, (count, LANES), 1)
    pair, lower = lane // (2 * WIDTH), lane % (2 * WIDTH) < WIDTH
    sums = [jnp.zeros((count, LANES), jnp.float32)] * 2
    for x, value in planes:
        m, k = x // 2, x % 2
        moved = pltpu.roll(value, (2 * WIDTH * m + WIDTH) % LANES, 1)
        sums[k] = jnp.where(pair == m, moved, sums[k])
    up = jnp.where(lower, sums[0], pltpu.roll(sums[1], WIDTH, 1))
    down = jnp.where(lower, pltpu.roll(sums[0], LANES - WIDTH, 1), sums[1])
    return up, down


def faces(odd, own, to_odd, to_even, nx):
    a = jnp.where(odd > 0, nx - WIDTH, 0)
    b = jnp.where(odd > 0, 0, nx - WIDTH)
    for i in range(WIDTH):
        to_odd[i] = own[a + i]
        to_even[i] = own[b + i]


def pack_y(reach, place, *refs):
    *own, one, slid, three, up, down = refs
    crossed = place[1]
    rows, total = one.shape[1], one.shape[0]

    def wide(src):
        for i in range(total):
            up[reach * i : reach * (i + 1)] = src[i, rows - reach : rows, :]
            down[reach * i : reach * (i + 1)] = src[i, 0:reach, :]

    @pl.when(crossed > 0)
    def _():
        wide(slid)

    @pl.when(crossed == 0)
    def _():
        wide(one)

    at = reach * total
    for src in (three, *own):
        for i in range(src.shape[0]):
            up[at : at + WIDTH] = src[i, rows - WIDTH : rows, :]
            down[at : at + WIDTH] = src[i, 0:WIDTH, :]
            at += WIDTH


def planes_of(q, nx, depths, own, sides):
    depth, at, total = depths[q], sum(depths[:q]), sum(depths)
    low = [(WIDTH - depth + i, sides, at + i, None) for i in range(depth)]
    mid = [(WIDTH + i, own, q * nx + i, q * nx + i) for i in range(nx)]
    high = [(WIDTH + nx + i, sides, total + at + i, None) for i in range(depth)]
    return low + mid + high


def pack_z(depths, nx, reach, place, *refs):
    *own, one, slid, three, ylo, yhi, sides, up, down, joined = refs
    rows, total = one.shape[1], one.shape[0]
    odd, crossed, start = place[0], place[1], place[2]
    high = rows + 2 * EDGE
    later = WIDTH * total + reach * total
    early = len(own) > 1

    def framed(src, base, i, below, above):
        at = base * total + i
        sides[at, EDGE : EDGE + rows] = src[i]
        sides[at, EDGE - WIDTH : EDGE] = ylo[below : below + WIDTH]
        sides[at, EDGE + rows : EDGE + rows + WIDTH] = yhi[above : above + WIDTH]

    for i in range(total):
        framed(three, 1 - odd, i, reach * total + WIDTH * i, reach * total + WIDTH * i)

    @pl.when(crossed > 0)
    def _():
        for i in range(total):
            joined[i, 0:reach] = ylo[reach * i : reach * (i + 1)]
            joined[i, reach : reach + rows] = slid[i]
            joined[i, reach + rows :] = yhi[reach * i : reach * (i + 1)]
        for i in range(total):
            sides[odd * total + i] = joined[i, pl.ds(start, high)]

    @pl.when(crossed == 0)
    def _():
        for i in range(total):
            framed(one, odd, i, reach * (i + 1) - WIDTH, reach * i)

    lane = lax.broadcasted_iota(jnp.int32, (32, LANES), 1)
    inside = (lane >= WIDTH * WIDTH) & (lane < WIDTH * (WIDTH + nx))
    for q in range(len(depths)):
        planes = planes_of(q, nx, depths, own[0], sides)
        for row, count in [(EDGE + r, 32) for r in range(0, rows, 32)] + [(EDGE - WIDTH, WIDTH), (EDGE + rows, WIDTH)]:
            values = []
            for x, src, index, p in planes:
                if p is None:
                    values.append((x, src[index, row : row + count]))
                elif count == WIDTH and early:
                    values.append((x, own[0 if row < EDGE else 1][p]))
                elif count == WIDTH:
                    values.append((x, (ylo if row < EDGE else yhi)[later + WIDTH * p : later + WIDTH * (p + 1)]))
                elif not early:
                    values.append((x, src[index, row - EDGE : row - EDGE + count]))
            high_lanes, low_lanes = pack_lanes(values, count)
            if early and count > WIDTH:
                at = slice(row - EDGE, row - EDGE + count)
                high_lanes = jnp.where(inside, own[2][q, at], high_lanes)
                low_lanes = jnp.where(inside, own[3][q, at], low_lanes)
            up[q, row : row + count] = high_lanes
            down[q, row : row + count] = low_lanes


def derive(read, write):
    d = read(1)
    v = [read(2 + k) for k in range(3)]
    write(0, 1.0 - 6.0 * d - (v[0] + v[1] + v[2]))
    for k in range(3):
        write(1 + 2 * k, d + jnp.maximum(v[k], 0.0))
        write(2 + 2 * k, d + jnp.minimum(v[k], 0.0))


def advance(second, *refs):
    odd_ref, own = refs[0], refs[1]
    halo = refs[2:7]
    refs = refs[7:]
    if second:
        field_own, field_halo, depths = refs[0], refs[1:6], (WIDTH,)
        out = refs[6]
        refs = refs[7:]
    else:
        field_own, field_halo, depths = own, halo, DEPTHS
        out, to_odd, to_even = refs[:3]
        refs = refs[3:]
    nx = out.shape[0]
    cells, coef, strip, strip_coef = refs
    rows = own.shape[1]
    high = rows + 2 * EDGE
    shift = PAD - EDGE

    for x, src, index, p in planes_of(0, nx, depths, field_own, field_halo[0]):
        if p is None:
            cells[0, x, shift : shift + high] = src[index]
            continue
        cells[0, x, PAD : PAD + rows] = src[index]
        at = field_halo[1].shape[0] - WIDTH * (nx - p)
        rim = (slice(at, at + WIDTH),) if second else (p,)
        cells[0, x, PAD - WIDTH : PAD] = field_halo[1][rim]
        cells[0, x, PAD + rows : PAD + rows + WIDTH] = field_halo[2][rim]
    for side in range(2):
        strip[0, side, shift : shift + high] = field_halo[3 + side][0]

        def write(k, value, side=side):
            strip_coef[k, side] = value

        derive(lambda q, side=side: halo[3 + side][q], write)
    for four in zip(*[planes_of(q, nx, DEPTHS, own, halo[0]) for q in range(1, 5)]):
        x, p = four[0][0], four[0][3]

        def at(row, count, x=x):
            def write(k, value):
                coef[k, x, row : row + count] = value

            return write

        offset = 0 if p is None else EDGE
        for r in range(0, high if p is None else rows, 16):
            derive(lambda q, r=r, four=four: four[q - 1][1][four[q - 1][2], r : r + 16], at(offset + r, 16))
        if p is not None:
            derive(lambda q, four=four: halo[1][four[q - 1][3]], at(EDGE - WIDTH, WIDTH))
            derive(lambda q, four=four: halo[2][four[q - 1][3]], at(EDGE + rows, WIDTH))

    for step in range(1, WIDTH + 1):
        src, dst = (step - 1) % 2, step % 2
        last = step == WIDTH
        size = rows // 2 if last else high // 2
        for row in (EDGE, EDGE + size) if last else (0, size):
            here = shift + row
            lane = lax.broadcasted_iota(jnp.int32, (size, LANES), 1)
            start, end = lane == 0, lane == LANES - 1
            group, place = lane // WIDTH, lane % WIDTH
            low, top = (strip[src, side, here : here + size] for side in range(2))
            beyond = jnp.where(place == WIDTH - 1, low, pltpu.roll(top, WIDTH - 2, 1))
            inner = jnp.zeros((size, LANES), jnp.float32)
            before = cells[src, step - 1, here : here + size]
            mid = cells[src, step, here : here + size]
            for x in range(step, nx + 2 * WIDTH - step):
                after = cells[src, x + 1, here : here + size]
                turn = WIDTH * x + WIDTH - 1
                outer = pltpu.roll(beyond, (LANES - turn) % LANES, 1)
                if not last:
                    inner = jnp.where(group == x, pltpu.roll(mid, turn % LANES, 1), inner)
                c = [coef[k, x, row : row + size] for k in range(7)]
                new = c[0] * mid + c[1] * before + c[2] * after
                new += c[3] * cells[src, x, here - 1 : here - 1 + size]
                new += c[4] * cells[src, x, here + 1 : here + 1 + size]
                new += c[5] * jnp.where(start, outer, pltpu.roll(mid, 1, 1))
                new += c[6] * jnp.where(end, outer, pltpu.roll(mid, LANES - 1, 1))
                if last:
                    out[x - WIDTH, row - EDGE : row - EDGE + size] = new
                else:
                    cells[dst, x, here : here + size] = new
                before, mid = mid, after
            if last:
                continue
            for side in range(2):
                mid = low if side == 0 else top
                below, above = pltpu.roll(mid, 1, 1), pltpu.roll(mid, LANES - 1, 1)
                if side == 0:
                    above = jnp.where(place == WIDTH - 1, inner, above)
                else:
                    below = jnp.where(place == 0, pltpu.roll(inner, LANES - (WIDTH - 2), 1), below)
                c = [strip_coef[k, side, row : row + size] for k in range(7)]
                new = c[0] * mid + c[1] * pltpu.roll(mid, WIDTH, 1) + c[2] * pltpu.roll(mid, LANES - WIDTH, 1)
                new += c[3] * strip[src, side, here - 1 : here - 1 + size]
                new += c[4] * strip[src, side, here + 1 : here + 1 + size]
                new += c[5] * below + c[6] * above
                strip[dst, side, here : here + size] = new
    if not second:
        faces(odd_ref[0], out, to_odd, to_even, nx)


def exchange_x(to_odd, to_even, shift, beside, args):
    count_x, count_y = lax.axis_size("gx"), lax.axis_size("gy")
    even = [(i, i + 1) for i in range(0, count_x, 2)]
    odd = [(i * count_y + j, (i + 1) * count_y + j) for i in range(1, count_x - 1, 2) for j in range(count_y)]
    odd += [(i * count_y + j, i * count_y + j + 1) for i in (0, count_x - 1) for j in range(0, count_y, 2)]

    def slide(k):
        pairs = []
        for j in range(count_y):
            top = (count_x - 1) * count_y + (j + k) % count_y
            pairs += [(j, top), (top, j)]
        return lambda a, *rest: (lax.ppermute(a, ("gx", "gy"), pairs), *beside(*rest))

    three = lax.ppermute(to_even, "gx", even + [(b, a) for a, b in even])
    one = lax.ppermute(to_odd, ("gx", "gy"), odd + [(b, a) for a, b in odd])
    slid, *rest = lax.switch(shift, [slide(k) for k in range(count_y)], to_odd, *args)
    return one, slid, three, rest


def shift_both(axis, up, down):
    n = lax.axis_size(axis)
    forth = [(i, (i + 1) % n) for i in range(n)]
    return lax.ppermute(up, axis, forth), lax.ppermute(down, axis, [(b, a) for a, b in forth])


def gather_halo(own, depths, to_odd, to_even, shift, place, inputs=None):
    total, rows, _ = to_odd.shape
    nx = own.shape[0] if inputs is None else inputs[0].shape[0]
    high = rows + 2 * EDGE
    reach = rows // 2 + EDGE

    def beside(*inputs):
        rim, lanes = (len(depths) * nx, WIDTH, LANES), (len(depths), rows, LANES)
        shapes = [(len(depths) * nx, rows, LANES), rim, rim, lanes, lanes]
        own, up, down, z_up, z_down = call(prepare, shapes, inputs)
        return own, *shift_both("gy", up, down), z_up, z_down

    if inputs is None:
        one, slid, three, _ = exchange_x(to_odd, to_even, shift, lambda: (), [])
        held, count = [own], reach * total + WIDTH * total + WIDTH * nx
    else:
        one, slid, three, (own, *held) = exchange_x(to_odd, to_even, shift, beside, inputs)
        count = reach * total + WIDTH * total
    first = held if inputs is None else []
    up, down = call(functools.partial(pack_y, reach), [(count, LANES)] * 2, [place, *first, one, slid, three], (), 1)
    ylo, yhi = shift_both("gy", up, down)
    shape = (len(depths), high, LANES)
    sides, up, down = call(
        functools.partial(pack_z, depths, nx, reach),
        [(2 * total, high, LANES), shape, shape],
        [place, *held, one, slid, three, ylo, yhi],
        [(total, rows + 2 * reach, LANES)],
        1,
    )
    zlo, zhi = shift_both("gz", up, down)
    if inputs is not None:
        ylo, yhi = held[:2]
    return own, [sides, ylo, yhi, zlo, zhi]


def body(concentration, speed, signs, diffusivity, shear):
    nx, rows, lanes = concentration.shape
    count_x, count_y = lax.axis_size("gx"), lax.axis_size("gy")
    x_index = lax.axis_index("gx")
    blocks = (shear[0] + rows // 2) // rows
    shift, rest = blocks % count_y, shear[0] - blocks * rows
    crossed = (x_index == 0) | (x_index == count_x - 1)
    start = rows // 2 + jnp.where(x_index == 0, rest, -rest)
    odd = (x_index % 2).astype(jnp.int32).reshape(1)
    place = jnp.stack([x_index % 2, crossed.astype(jnp.int32), jnp.where(crossed, start, 0)]).astype(jnp.int32)
    face = (sum(DEPTHS), rows, lanes)
    inputs = [concentration, speed, signs, diffusivity]
    short = (2, WIDTH - 1, rows, lanes)
    to_odd, to_even = pl.pallas_call(
        first_faces,
        out_shape=[jax.ShapeDtypeStruct(face, jnp.float32)] * 2,
        in_specs=[SMEM] + [pl.BlockSpec(memory_space=pl.ANY)] * 4,
        out_specs=[VMEM] * 2,
        scratch_shapes=[
            pltpu.VMEM((2, WIDTH, rows, lanes), jnp.float32),
            pltpu.VMEM((2, 3, *short[1:]), jnp.float32),
            pltpu.VMEM((2, 3, *short[1:]), jnp.int32),
            pltpu.VMEM(short, jnp.float32),
            pltpu.SemaphoreType.DMA((8,)),
        ],
        compiler_params=pltpu.CompilerParams(vmem_limit_bytes=8 * 2**20),
    )(odd, *inputs)
    own, halo = gather_halo(None, DEPTHS, to_odd, to_even, shift, place, inputs)
    high = rows + 2 * EDGE
    wide = nx + 2 * WIDTH
    scratch = [(2, wide, rows + 2 * PAD, lanes), (7, wide, high, lanes), (2, 2, rows + 2 * PAD, lanes), (7, 2, high, lanes)]
    face = (WIDTH, rows, lanes)
    field, to_odd, to_even = call(
        functools.partial(advance, False), [(nx, rows, lanes), face, face], [odd, own] + halo, scratch, 1
    )
    field, later = gather_halo(field, (WIDTH,), to_odd, to_even, shift, place)
    (field,) = call(functools.partial(advance, True), [(nx, rows, lanes)], [odd, own] + halo + [field] + later, scratch, 1)
    return field


def solution(mesh):
    placed = (
        P("gx", "gy", "gz"),
        P(None, "gx", "gy", "gz"),
        P(None, "gx", "gy", "gz"),
        P("gx", "gy", "gz"),
        P(),
    )
    return jax.shard_map(
        body, mesh=mesh, in_specs=placed, out_specs=P("gx", "gy", "gz"), check_vma=False
    )
```

```python
import functools
import math

import jax
import jax.numpy as jnp
from jax import lax
from jax.experimental import pallas as pl
from jax.experimental.pallas import tpu as pltpu
from jax.sharding import PartitionSpec as P

STEPS = 8
WIDTH = 4
TIME_STEP = 0.25
PAD = 16
EDGE = 8
LANES = 128

VMEM = pl.BlockSpec(memory_space=pltpu.VMEM)
SMEM = pl.BlockSpec(memory_space=pltpu.SMEM)
DEPTHS = (WIDTH, WIDTH - 1, WIDTH - 1, WIDTH - 1, WIDTH - 1)


def call(kernel, outs, args, scratch=(), scalars=0):
    need = sum(4 * math.prod(shape) for shape in list(outs) + list(scratch))
    need += sum(4 * math.prod(arg.shape) for arg in args[scalars:])
    return pl.pallas_call(
        kernel,
        out_shape=[jax.ShapeDtypeStruct(shape, jnp.float32) for shape in outs],
        in_specs=[SMEM] * scalars + [VMEM] * (len(args) - scalars),
        out_specs=[VMEM] * len(outs),
        scratch_shapes=[pltpu.VMEM(shape, jnp.float32) for shape in scratch],
        compiler_params=pltpu.CompilerParams(vmem_limit_bytes=need + 4 * 2**20),
    )(*args)


def first_faces(odd_ref, field, speed, signs, diffusivity, to_odd, to_even, f, s, g, d, sems):
    nx = field.shape[0]
    copies = []
    for side in range(2):
        deep, short = (pl.ds(nx - n if side else 0, n) for n in DEPTHS[:2])
        for src, dst in (
            (field.at[deep], f.at[side]),
            (diffusivity.at[short], d.at[side]),
            (speed.at[:, short], s.at[side]),
            (signs.at[:, short], g.at[side]),
        ):
            copies.append(pltpu.make_async_copy(src, dst, sems.at[len(copies)]))
    for copy in copies:
        copy.start()
    for copy in copies:
        copy.wait()
    odd = odd_ref[0]
    for out, side in ((to_odd, odd), (to_even, 1 - odd)):
        for i in range(WIDTH):
            out[i] = f[side, i]
        for i in range(WIDTH - 1):
            out[WIDTH + i] = TIME_STEP * d[side, i]
            for k in range(3):
                scaled = TIME_STEP * s[side, k, i]
                out[WIDTH + (1 + k) * (WIDTH - 1) + i] = jnp.where(g[side, k, i] > 0, scaled, -scaled)


def prepare(field, speed, signs, diffusivity, own, y_up, y_down, z_up, z_down):
    nx, rows = field.shape[:2]

    def plane(x, carry):
        own[x] = field[x]
        own[nx + x] = TIME_STEP * diffusivity[x]
        for d in range(3):
            scaled = TIME_STEP * speed[d, x]
            own[(2 + d) * nx + x] = jnp.where(signs[d, x] > 0, scaled, -scaled)
        return carry

    lax.fori_loop(0, nx, plane, 0)

    def edge(p, carry):
        y_up[p] = own[p, rows - WIDTH : rows, :]
        y_down[p] = own[p, 0:WIDTH, :]
        return carry

    lax.fori_loop(0, own.shape[0], edge, 0)

    def quantity(q, carry):
        for row in range(0, rows, 32):
            planes = [(WIDTH + i, own[q * nx + i, row : row + 32]) for i in range(nx)]
            up, down = pack_lanes(planes, 32)
            z_up[q, row : row + 32] = up
            z_down[q, row : row + 32] = down
        return carry

    lax.fori_loop(0, z_up.shape[0], quantity, 0)


def pack_lanes(planes, count):
    lane = lax.broadcasted_iota(jnp.int32, (count, LANES), 1)
    pair, lower = lane // (2 * WIDTH), lane % (2 * WIDTH) < WIDTH
    sums = [jnp.zeros((count, LANES), jnp.float32)] * 2
    for x, value in planes:
        m, k = x // 2, x % 2
        moved = pltpu.roll(value, (2 * WIDTH * m + WIDTH) % LANES, 1)
        sums[k] = jnp.where(pair == m, moved, sums[k])
    up = jnp.where(lower, sums[0], pltpu.roll(sums[1], WIDTH, 1))
    down = jnp.where(lower, pltpu.roll(sums[0], LANES - WIDTH, 1), sums[1])
    return up, down


def faces(odd, own, to_odd, to_even, nx):
    a = jnp.where(odd > 0, nx - WIDTH, 0)
    b = jnp.where(odd > 0, 0, nx - WIDTH)
    for i in range(WIDTH):
        to_odd[i] = own[a + i]
        to_even[i] = own[b + i]


def pack_y(reach, place, *refs):
    *own, one, slid, three, up, down = refs
    crossed = place[1]
    rows, total = one.shape[1], one.shape[0]

    def wide(src):
        for i in range(total):
            up[reach * i : reach * (i + 1)] = src[i, rows - reach : rows, :]
            down[reach * i : reach * (i + 1)] = src[i, 0:reach, :]

    @pl.when(crossed > 0)
    def _():
        wide(slid)

    @pl.when(crossed == 0)
    def _():
        wide(one)

    at = reach * total
    for src in (three, *own):
        for i in range(src.shape[0]):
            up[at : at + WIDTH] = src[i, rows - WIDTH : rows, :]
            down[at : at + WIDTH] = src[i, 0:WIDTH, :]
            at += WIDTH


def planes_of(q, nx, depths, own, sides):
    depth, at, total = depths[q], sum(depths[:q]), sum(depths)
    low = [(WIDTH - depth + i, sides, at + i, None) for i in range(depth)]
    mid = [(WIDTH + i, own, q * nx + i, q * nx + i) for i in range(nx)]
    high = [(WIDTH + nx + i, sides, total + at + i, None) for i in range(depth)]
    return low + mid + high


def place_sides(reach, place, one, slid, three, ylo, yhi, sides, joined):
    rows, total = one.shape[1], one.shape[0]
    odd, crossed, start = place[0], place[1], place[2]

    def framed(src, base, i, below, above):
        at = base * total + i
        sides[at, EDGE : EDGE + rows] = src[i]
        sides[at, EDGE - WIDTH : EDGE] = ylo[below : below + WIDTH]
        sides[at, EDGE + rows : EDGE + rows + WIDTH] = yhi[above : above + WIDTH]

    for i in range(total):
        framed(three, 1 - odd, i, reach * total + WIDTH * i, reach * total + WIDTH * i)

    @pl.when(crossed > 0)
    def _():
        for i in range(total):
            joined[i, 0:reach] = ylo[reach * i : reach * (i + 1)]
            joined[i, reach : reach + rows] = slid[i]
            joined[i, reach + rows :] = yhi[reach * i : reach * (i + 1)]
        for i in range(total):
            sides[odd * total + i, EDGE - WIDTH : EDGE + rows + WIDTH] = joined[i, pl.ds(start, rows + 2 * WIDTH)]

    @pl.when(crossed == 0)
    def _():
        for i in range(total):
            framed(one, odd, i, reach * (i + 1) - WIDTH, reach * i)


def pack_own_rims(ylo, yhi, z_up, z_down, up, down):
    rows = z_up.shape[1]
    nx = ylo.shape[0] // z_up.shape[0]
    for q in range(z_up.shape[0]):
        for row, rim in ((EDGE - WIDTH, ylo), (EDGE + rows, yhi)):
            last, first = pack_lanes([(WIDTH + i, rim[q * nx + i]) for i in range(nx)], WIDTH)
            up[q, row : row + WIDTH] = last
            down[q, row : row + WIDTH] = first
        up[q, EDGE : EDGE + rows] = z_up[q]
        down[q, EDGE : EDGE + rows] = z_down[q]


def side_slots(depths):
    return [(2 * sum(depths[:q]), depth) for q, depth in enumerate(depths)]


def pack_sides(depths, reach, place, *refs):
    one, slid, three, ylo, yhi, sides, up, down, joined = refs
    place_sides(reach, place, one, slid, three, ylo, yhi, sides, joined)
    total = one.shape[0]
    for row in range(0, up.shape[0], 16):
        values = []
        for q, (slot, depth) in enumerate(side_slots(depths)):
            for i in range(depth):
                at = sum(depths[:q]) + i
                values.append((slot + i, sides[at, row : row + 16]))
                values.append((slot + depth + i, sides[total + at, row : row + 16]))
        up[row : row + 16], down[row : row + 16] = pack_lanes(values, 16)


def pack_z(depths, nx, reach, place, *refs):
    own, one, slid, three, ylo, yhi, sides, up, down, joined = refs
    place_sides(reach, place, one, slid, three, ylo, yhi, sides, joined)
    rows, total = one.shape[1], one.shape[0]
    later = WIDTH * total + reach * total
    for q in range(len(depths)):
        planes = planes_of(q, nx, depths, own, sides)
        for row, count in [(EDGE + r, 32) for r in range(0, rows, 32)] + [(EDGE - WIDTH, WIDTH), (EDGE + rows, WIDTH)]:
            values = []
            for x, src, index, p in planes:
                if p is None:
                    values.append((x, src[index, row : row + count]))
                elif count == WIDTH:
                    values.append((x, (ylo if row < EDGE else yhi)[later + WIDTH * p : later + WIDTH * (p + 1)]))
                else:
                    values.append((x, src[index, row - EDGE : row - EDGE + count]))
            up[q, row : row + count], down[q, row : row + count] = pack_lanes(values, count)


def derive(read, write):
    d = read(1)
    v = [read(2 + k) for k in range(3)]
    write(0, 1.0 - 6.0 * d - (v[0] + v[1] + v[2]))
    for k in range(3):
        write(1 + 2 * k, d + jnp.maximum(v[k], 0.0))
        write(2 + 2 * k, d + jnp.minimum(v[k], 0.0))


def advance(second, *refs):
    odd_ref, own = refs[0], refs[1]
    halo = refs[2:9]
    refs = refs[9:]
    if second:
        field_own, field_halo, depths = refs[0], refs[1:6], (WIDTH,)
        out = refs[6]
        refs = refs[7:]
    else:
        field_own, field_halo, depths = own, halo, DEPTHS
        out, to_odd, to_even = refs[:3]
        refs = refs[3:]
    nx = out.shape[0]
    cells, coef, strip, strip_coef = refs
    rows = own.shape[1]
    high = rows + 2 * EDGE
    shift = PAD - EDGE

    for x, src, index, p in planes_of(0, nx, depths, field_own, field_halo[0]):
        if p is None:
            cells[0, x, shift : shift + high] = src[index]
            continue
        cells[0, x, PAD : PAD + rows] = src[index]
        at = field_halo[1].shape[0] - WIDTH * (nx - p)
        rim = (slice(at, at + WIDTH),) if second else (p,)
        cells[0, x, PAD - WIDTH : PAD] = field_halo[1][rim]
        cells[0, x, PAD + rows : PAD + rows + WIDTH] = field_halo[2][rim]
    lane = lax.broadcasted_iota(jnp.int32, (high, LANES), 1)
    inside = (lane >= WIDTH * WIDTH) & (lane < WIDTH * (WIDTH + nx))
    slots = side_slots(DEPTHS)

    def z_halo(q, side):
        slot, depth = slots[q]
        packed = halo[5 + side][...]
        low = pltpu.roll(packed, WIDTH * (WIDTH - depth - slot) % LANES, 1)
        top = pltpu.roll(packed, WIDTH * (WIDTH + nx - slot - depth) % LANES, 1)
        return jnp.where(inside, halo[3 + side][q], jnp.where(lane < WIDTH * WIDTH, low, top))

    for side in range(2):
        strip[0, side, shift : shift + high] = field_halo[3 + side][0] if second else z_halo(0, side)

        def write(k, value, side=side):
            strip_coef[k, side] = value

        derive(functools.partial(z_halo, side=side), write)
    for four in zip(*[planes_of(q, nx, DEPTHS, own, halo[0]) for q in range(1, 5)]):
        x, p = four[0][0], four[0][3]

        def at(row, count, x=x):
            def write(k, value):
                coef[k, x, row : row + count] = value

            return write

        offset = 0 if p is None else EDGE
        for r in range(0, high if p is None else rows, 16):
            derive(lambda q, r=r, four=four: four[q - 1][1][four[q - 1][2], r : r + 16], at(offset + r, 16))
        if p is not None:
            derive(lambda q, four=four: halo[1][four[q - 1][3]], at(EDGE - WIDTH, WIDTH))
            derive(lambda q, four=four: halo[2][four[q - 1][3]], at(EDGE + rows, WIDTH))

    for step in range(1, WIDTH + 1):
        src, dst = (step - 1) % 2, step % 2
        last = step == WIDTH
        size = rows // 2 if last else high // 2
        for row in (EDGE, EDGE + size) if last else (0, size):
            here = shift + row
            lane = lax.broadcasted_iota(jnp.int32, (size, LANES), 1)
            start, end = lane == 0, lane == LANES - 1
            group, place = lane // WIDTH, lane % WIDTH
            low, top = (strip[src, side, here : here + size] for side in range(2))
            beyond = jnp.where(place == WIDTH - 1, low, pltpu.roll(top, WIDTH - 2, 1))
            inner = jnp.zeros((size, LANES), jnp.float32)
            before = cells[src, step - 1, here : here + size]
            mid = cells[src, step, here : here + size]
            for x in range(step, nx + 2 * WIDTH - step):
                after = cells[src, x + 1, here : here + size]
                turn = WIDTH * x + WIDTH - 1
                outer = pltpu.roll(beyond, (LANES - turn) % LANES, 1)
                if not last:
                    inner = jnp.where(group == x, pltpu.roll(mid, turn % LANES, 1), inner)
                c = [coef[k, x, row : row + size] for k in range(7)]
                new = c[0] * mid + c[1] * before + c[2] * after
                new += c[3] * cells[src, x, here - 1 : here - 1 + size]
                new += c[4] * cells[src, x, here + 1 : here + 1 + size]
                new += c[5] * jnp.where(start, outer, pltpu.roll(mid, 1, 1))
                new += c[6] * jnp.where(end, outer, pltpu.roll(mid, LANES - 1, 1))
                if last:
                    out[x - WIDTH, row - EDGE : row - EDGE + size] = new
                else:
                    cells[dst, x, here : here + size] = new
                before, mid = mid, after
            if last:
                continue
            for side in range(2):
                mid = low if side == 0 else top
                below, above = pltpu.roll(mid, 1, 1), pltpu.roll(mid, LANES - 1, 1)
                if side == 0:
                    above = jnp.where(place == WIDTH - 1, inner, above)
                else:
                    below = jnp.where(place == 0, pltpu.roll(inner, LANES - (WIDTH - 2), 1), below)
                c = [strip_coef[k, side, row : row + size] for k in range(7)]
                new = c[0] * mid + c[1] * pltpu.roll(mid, WIDTH, 1) + c[2] * pltpu.roll(mid, LANES - WIDTH, 1)
                new += c[3] * strip[src, side, here - 1 : here - 1 + size]
                new += c[4] * strip[src, side, here + 1 : here + 1 + size]
                new += c[5] * below + c[6] * above
                strip[dst, side, here : here + size] = new
    if not second:
        faces(odd_ref[0], out, to_odd, to_even, nx)


def exchange_x(to_odd, to_even, shift, beside, args):
    count_x, count_y = lax.axis_size("gx"), lax.axis_size("gy")
    even = [(i, i + 1) for i in range(0, count_x, 2)]
    odd = [(i * count_y + j, (i + 1) * count_y + j) for i in range(1, count_x - 1, 2) for j in range(count_y)]
    odd += [(i * count_y + j, i * count_y + j + 1) for i in (0, count_x - 1) for j in range(0, count_y, 2)]

    def slide(k):
        pairs = []
        for j in range(count_y):
            top = (count_x - 1) * count_y + (j + k) % count_y
            pairs += [(j, top), (top, j)]
        return lambda a, *rest: (lax.ppermute(a, ("gx", "gy"), pairs), *beside(*rest))

    three = lax.ppermute(to_even, "gx", even + [(b, a) for a, b in even])
    one = lax.ppermute(to_odd, ("gx", "gy"), odd + [(b, a) for a, b in odd])
    slid, *rest = lax.switch(shift, [slide(k) for k in range(count_y)], to_odd, *args)
    return one, slid, three, rest


def shift_both(axis, up, down):
    n = lax.axis_size(axis)
    forth = [(i, (i + 1) % n) for i in range(n)]
    return lax.ppermute(up, axis, forth), lax.ppermute(down, axis, [(b, a) for a, b in forth])


def first_halo(inputs, to_odd, to_even, shift, place):
    total, rows, _ = to_odd.shape
    nx, count = inputs[0].shape[0], len(DEPTHS)
    high = rows + 2 * EDGE
    reach = rows // 2 + WIDTH

    def beside(*inputs):
        rim, lanes = (count * nx, WIDTH, LANES), (count, rows, LANES)
        own, up, down, z_up, z_down = call(prepare, [(count * nx, rows, LANES), rim, rim, lanes, lanes], inputs)
        return own, *shift_both("gy", up, down), z_up, z_down

    one, slid, three, (own, y_low, y_high, z_up, z_down) = exchange_x(to_odd, to_even, shift, beside, inputs)
    shape = (reach * total + WIDTH * total, LANES)
    up, down = call(functools.partial(pack_y, reach), [shape] * 2, [place, one, slid, three], (), 1)
    up, down, z_up, z_down = lax.optimization_barrier((up, down, z_up, z_down))
    ylo, yhi = shift_both("gy", up, down)
    z_up, z_down = call(pack_own_rims, [(count, high, LANES)] * 2, [y_low, y_high, z_up, z_down])
    z_low, z_high = shift_both("gz", z_up, z_down)
    sides, up, down = call(
        functools.partial(pack_sides, DEPTHS, reach),
        [(2 * total, high, LANES), (high, LANES), (high, LANES)],
        [place, one, slid, three, ylo, yhi],
        [(total, rows + 2 * reach, LANES)],
        1,
    )
    return own, [sides, y_low, y_high, z_low, z_high, *shift_both("gz", up, down)]


def second_halo(field, to_odd, to_even, shift, place):
    total, rows, _ = to_odd.shape
    nx = field.shape[0]
    reach = rows // 2 + WIDTH
    high = rows + 2 * EDGE
    one, slid, three, _ = exchange_x(to_odd, to_even, shift, lambda: (), [])
    shape = (reach * total + WIDTH * total + WIDTH * nx, LANES)
    up, down = call(functools.partial(pack_y, reach), [shape] * 2, [place, field, one, slid, three], (), 1)
    ylo, yhi = shift_both("gy", up, down)
    shape = (1, high, LANES)
    sides, up, down = call(
        functools.partial(pack_z, (WIDTH,), nx, reach),
        [(2 * total, high, LANES), shape, shape],
        [place, field, one, slid, three, ylo, yhi],
        [(total, rows + 2 * reach, LANES)],
        1,
    )
    return [sides, ylo, yhi, *shift_both("gz", up, down)]


def body(concentration, speed, signs, diffusivity, shear):
    nx, rows, lanes = concentration.shape
    count_x, count_y = lax.axis_size("gx"), lax.axis_size("gy")
    x_index = lax.axis_index("gx")
    blocks = (shear[0] + rows // 2) // rows
    shift, rest = blocks % count_y, shear[0] - blocks * rows
    crossed = (x_index == 0) | (x_index == count_x - 1)
    start = rows // 2 + jnp.where(x_index == 0, rest, -rest)
    odd = (x_index % 2).astype(jnp.int32).reshape(1)
    place = jnp.stack([x_index % 2, crossed.astype(jnp.int32), jnp.where(crossed, start, 0)]).astype(jnp.int32)
    face = (sum(DEPTHS), rows, lanes)
    inputs = [concentration, speed, signs, diffusivity]
    short = (2, WIDTH - 1, rows, lanes)
    to_odd, to_even = pl.pallas_call(
        first_faces,
        out_shape=[jax.ShapeDtypeStruct(face, jnp.float32)] * 2,
        in_specs=[SMEM] + [pl.BlockSpec(memory_space=pl.ANY)] * 4,
        out_specs=[VMEM] * 2,
        scratch_shapes=[
            pltpu.VMEM((2, WIDTH, rows, lanes), jnp.float32),
            pltpu.VMEM((2, 3, *short[1:]), jnp.float32),
            pltpu.VMEM((2, 3, *short[1:]), jnp.int32),
            pltpu.VMEM(short, jnp.float32),
            pltpu.SemaphoreType.DMA((8,)),
        ],
        compiler_params=pltpu.CompilerParams(vmem_limit_bytes=8 * 2**20),
    )(odd, *inputs)
    own, halo = first_halo(inputs, to_odd, to_even, shift, place)
    high = rows + 2 * EDGE
    wide = nx + 2 * WIDTH
    scratch = [(2, wide, rows + 2 * PAD, lanes), (7, wide, high, lanes), (2, 2, rows + 2 * PAD, lanes), (7, 2, high, lanes)]
    face = (WIDTH, rows, lanes)
    field, to_odd, to_even = call(
        functools.partial(advance, False), [(nx, rows, lanes), face, face], [odd, own] + halo, scratch, 1
    )
    later = second_halo(field, to_odd, to_even, shift, place)
    (field,) = call(functools.partial(advance, True), [(nx, rows, lanes)], [odd, own] + halo + [field] + later, scratch, 1)
    return field


def solution(mesh):
    placed = (
        P("gx", "gy", "gz"),
        P(None, "gx", "gy", "gz"),
        P(None, "gx", "gy", "gz"),
        P("gx", "gy", "gz"),
        P(),
    )
    return jax.shard_map(
        body, mesh=mesh, in_specs=placed, out_specs=P("gx", "gy", "gz"), check_vma=False
    )
```

```python
import functools
import math

import jax
import jax.numpy as jnp
from jax import lax
from jax.experimental import pallas as pl
from jax.experimental.pallas import tpu as pltpu
from jax.sharding import PartitionSpec as P

STEPS = 8
WIDTH = 4
TIME_STEP = 0.25
PAD = 16
EDGE = 8
LANES = 128

VMEM = pl.BlockSpec(memory_space=pltpu.VMEM)
SMEM = pl.BlockSpec(memory_space=pltpu.SMEM)
DEPTHS = (WIDTH, WIDTH - 1, WIDTH - 1, WIDTH - 1, WIDTH - 1)


def call(kernel, outs, args, scratch=(), scalars=0):
    need = sum(4 * math.prod(shape) for shape in list(outs) + list(scratch))
    need += sum(4 * math.prod(arg.shape) for arg in args[scalars:])
    return pl.pallas_call(
        kernel,
        out_shape=[jax.ShapeDtypeStruct(shape, jnp.float32) for shape in outs],
        in_specs=[SMEM] * scalars + [VMEM] * (len(args) - scalars),
        out_specs=[VMEM] * len(outs),
        scratch_shapes=[pltpu.VMEM(shape, jnp.float32) for shape in scratch],
        compiler_params=pltpu.CompilerParams(vmem_limit_bytes=need + 4 * 2**20),
    )(*args)


def first_faces(odd_ref, field, speed, signs, diffusivity, to_odd, to_even, f, s, g, d, sems):
    nx = field.shape[0]
    copies = []
    for side in range(2):
        deep, short = (pl.ds(nx - n if side else 0, n) for n in DEPTHS[:2])
        for src, dst in (
            (field.at[deep], f.at[side]),
            (diffusivity.at[short], d.at[side]),
            (speed.at[:, short], s.at[side]),
            (signs.at[:, short], g.at[side]),
        ):
            copies.append(pltpu.make_async_copy(src, dst, sems.at[len(copies)]))
    for copy in copies:
        copy.start()
    for copy in copies:
        copy.wait()
    odd = odd_ref[0]
    for out, side in ((to_odd, odd), (to_even, 1 - odd)):
        for i in range(WIDTH):
            out[i] = f[side, i]
        for i in range(WIDTH - 1):
            out[WIDTH + i] = TIME_STEP * d[side, i]
            for k in range(3):
                scaled = TIME_STEP * s[side, k, i]
                out[WIDTH + (1 + k) * (WIDTH - 1) + i] = jnp.where(g[side, k, i] > 0, scaled, -scaled)


def prepare(field, speed, signs, diffusivity, own, y_up, y_down, z_up, z_down):
    nx, rows = field.shape[:2]

    def plane(x, carry):
        own[x] = field[x]
        own[nx + x] = TIME_STEP * diffusivity[x]
        for d in range(3):
            scaled = TIME_STEP * speed[d, x]
            own[(2 + d) * nx + x] = jnp.where(signs[d, x] > 0, scaled, -scaled)
        return carry

    lax.fori_loop(0, nx, plane, 0)

    def edge(p, carry):
        y_up[p] = own[p, rows - WIDTH : rows, :]
        y_down[p] = own[p, 0:WIDTH, :]
        return carry

    lax.fori_loop(0, own.shape[0], edge, 0)

    def quantity(q, carry):
        for row in range(0, rows, 32):
            planes = [(WIDTH + i, own[q * nx + i, row : row + 32]) for i in range(nx)]
            up, down = pack_lanes(planes, 32)
            z_up[q, row : row + 32] = up
            z_down[q, row : row + 32] = down
        return carry

    lax.fori_loop(0, z_up.shape[0], quantity, 0)


def pack_lanes(planes, count):
    lane = lax.broadcasted_iota(jnp.int32, (count, LANES), 1)
    pair, lower = lane // (2 * WIDTH), lane % (2 * WIDTH) < WIDTH
    sums = [jnp.zeros((count, LANES), jnp.float32)] * 2
    for x, value in planes:
        m, k = x // 2, x % 2
        moved = pltpu.roll(value, (2 * WIDTH * m + WIDTH) % LANES, 1)
        sums[k] = jnp.where(pair == m, moved, sums[k])
    up = jnp.where(lower, sums[0], pltpu.roll(sums[1], WIDTH, 1))
    down = jnp.where(lower, pltpu.roll(sums[0], LANES - WIDTH, 1), sums[1])
    return up, down


def faces(odd, own, to_odd, to_even, nx):
    a = jnp.where(odd > 0, nx - WIDTH, 0)
    b = jnp.where(odd > 0, 0, nx - WIDTH)
    for i in range(WIDTH):
        to_odd[i] = own[a + i]
        to_even[i] = own[b + i]


def pack_y(reach, place, *refs):
    *own, one, slid, three, up, down = refs
    crossed = place[1]
    rows, total = one.shape[1], one.shape[0]

    def wide(src):
        for i in range(total):
            up[reach * i : reach * (i + 1)] = src[i, rows - reach : rows, :]
            down[reach * i : reach * (i + 1)] = src[i, 0:reach, :]

    @pl.when(crossed > 0)
    def _():
        wide(slid)

    @pl.when(crossed == 0)
    def _():
        wide(one)

    at = reach * total
    for src in (three, *own):
        for i in range(src.shape[0]):
            up[at : at + WIDTH] = src[i, rows - WIDTH : rows, :]
            down[at : at + WIDTH] = src[i, 0:WIDTH, :]
            at += WIDTH


def planes_of(q, nx, depths, own, sides):
    depth, at, total = depths[q], sum(depths[:q]), sum(depths)
    low = [(WIDTH - depth + i, sides, at + i, None) for i in range(depth)]
    mid = [(WIDTH + i, own, q * nx + i, q * nx + i) for i in range(nx)]
    high = [(WIDTH + nx + i, sides, total + at + i, None) for i in range(depth)]
    return low + mid + high


def place_sides(reach, place, one, slid, three, ylo, yhi, sides, joined):
    rows, total = one.shape[1], one.shape[0]
    odd, crossed, start = place[0], place[1], place[2]

    def framed(src, base, i, below, above):
        at = base * total + i
        sides[at, EDGE : EDGE + rows] = src[i]
        sides[at, EDGE - WIDTH : EDGE] = ylo[below : below + WIDTH]
        sides[at, EDGE + rows : EDGE + rows + WIDTH] = yhi[above : above + WIDTH]

    for i in range(total):
        framed(three, 1 - odd, i, reach * total + WIDTH * i, reach * total + WIDTH * i)

    @pl.when(crossed > 0)
    def _():
        for i in range(total):
            joined[i, 0:reach] = ylo[reach * i : reach * (i + 1)]
            joined[i, reach : reach + rows] = slid[i]
            joined[i, reach + rows :] = yhi[reach * i : reach * (i + 1)]
        for i in range(total):
            sides[odd * total + i, EDGE - WIDTH : EDGE + rows + WIDTH] = joined[i, pl.ds(start, rows + 2 * WIDTH)]

    @pl.when(crossed == 0)
    def _():
        for i in range(total):
            framed(one, odd, i, reach * (i + 1) - WIDTH, reach * i)


def pack_own_rims(ylo, yhi, z_up, z_down, up, down):
    rows = z_up.shape[1]
    nx = ylo.shape[0] // z_up.shape[0]
    for q in range(z_up.shape[0]):
        for row, rim in ((EDGE - WIDTH, ylo), (EDGE + rows, yhi)):
            last, first = pack_lanes([(WIDTH + i, rim[q * nx + i]) for i in range(nx)], WIDTH)
            up[q, row : row + WIDTH] = last
            down[q, row : row + WIDTH] = first
        up[q, EDGE : EDGE + rows] = z_up[q]
        down[q, EDGE : EDGE + rows] = z_down[q]


def side_slots(depths):
    return [(2 * sum(depths[:q]), depth) for q, depth in enumerate(depths)]


def pack_sides(depths, reach, place, *refs):
    one, slid, three, ylo, yhi, sides, up, down, joined = refs
    place_sides(reach, place, one, slid, three, ylo, yhi, sides, joined)
    total = one.shape[0]
    for row in range(0, up.shape[0], 16):
        values = []
        for q, (slot, depth) in enumerate(side_slots(depths)):
            for i in range(depth):
                at = sum(depths[:q]) + i
                values.append((slot + i, sides[at, row : row + 16]))
                values.append((slot + depth + i, sides[total + at, row : row + 16]))
        up[row : row + 16], down[row : row + 16] = pack_lanes(values, 16)


def pack_z(depths, nx, reach, place, *refs):
    own, one, slid, three, ylo, yhi, sides, up, down, joined = refs
    place_sides(reach, place, one, slid, three, ylo, yhi, sides, joined)
    rows, total = one.shape[1], one.shape[0]
    later = WIDTH * total + reach * total
    for q in range(len(depths)):
        planes = planes_of(q, nx, depths, own, sides)
        for row, count in [(EDGE + r, 32) for r in range(0, rows, 32)] + [(EDGE - WIDTH, WIDTH), (EDGE + rows, WIDTH)]:
            values = []
            for x, src, index, p in planes:
                if p is None:
                    values.append((x, src[index, row : row + count]))
                elif count == WIDTH:
                    values.append((x, (ylo if row < EDGE else yhi)[later + WIDTH * p : later + WIDTH * (p + 1)]))
                else:
                    values.append((x, src[index, row - EDGE : row - EDGE + count]))
            up[q, row : row + count], down[q, row : row + count] = pack_lanes(values, count)


def derive(read, write):
    d = read(1)
    v = [read(2 + k) for k in range(3)]
    write(0, 1.0 - 6.0 * d - (v[0] + v[1] + v[2]))
    for k in range(3):
        write(1 + 2 * k, d + jnp.maximum(v[k], 0.0))
        write(2 + 2 * k, d + jnp.minimum(v[k], 0.0))


def first_steps(odd_ref, own, sides, ylo, yhi, z_low, z_high, z_side_low, z_side_high, *refs):
    out, to_odd, to_even, coef, strip_coef, cells, strip = refs
    nx, rows = out.shape[:2]
    high = rows + 2 * EDGE
    shift = PAD - EDGE

    lay_field(planes_of(0, nx, DEPTHS, own, sides), cells, lambda p: ylo[p], lambda p: yhi[p], rows)
    lane = lax.broadcasted_iota(jnp.int32, (high, LANES), 1)
    inside = (lane >= WIDTH * WIDTH) & (lane < WIDTH * (WIDTH + nx))
    slots = side_slots(DEPTHS)
    z_own, z_sides = (z_low, z_high), (z_side_low, z_side_high)

    def z_halo(q, side):
        slot, depth = slots[q]
        packed = z_sides[side][...]
        low = pltpu.roll(packed, WIDTH * (WIDTH - depth - slot) % LANES, 1)
        top = pltpu.roll(packed, WIDTH * (WIDTH + nx - slot - depth) % LANES, 1)
        return jnp.where(inside, z_own[side][q], jnp.where(lane < WIDTH * WIDTH, low, top))

    for side in range(2):
        strip[0, side, shift : shift + high] = z_halo(0, side)

        def write(k, value, side=side):
            strip_coef[k, side] = value

        derive(functools.partial(z_halo, side=side), write)
    for four in zip(*[planes_of(q, nx, DEPTHS, own, sides) for q in range(1, 5)]):
        x, p = four[0][0], four[0][3]

        def at(row, count, x=x):
            def write(k, value):
                coef[k, x, row : row + count] = value

            return write

        offset = 0 if p is None else EDGE
        for r in range(0, high if p is None else rows, 16):
            derive(lambda q, r=r, four=four: four[q - 1][1][four[q - 1][2], r : r + 16], at(offset + r, 16))
        if p is not None:
            derive(lambda q, four=four: ylo[four[q - 1][3]], at(EDGE - WIDTH, WIDTH))
            derive(lambda q, four=four: yhi[four[q - 1][3]], at(EDGE + rows, WIDTH))
    advance(out, cells, coef, strip, strip_coef)
    faces(odd_ref[0], out, to_odd, to_even, nx)


def last_steps(field, coef, strip_coef, sides, ylo, yhi, z_low, z_high, out, cells, strip):
    nx, rows = out.shape[:2]
    shift = PAD - EDGE
    base = ylo.shape[0] - WIDTH * nx
    rim = lambda ref: lambda p: ref[base + WIDTH * p : base + WIDTH * (p + 1)]
    lay_field(planes_of(0, nx, (WIDTH,), field, sides), cells, rim(ylo), rim(yhi), rows)
    for side, ref in enumerate((z_low, z_high)):
        strip[0, side, shift : shift + rows + 2 * EDGE] = ref[0]
    advance(out, cells, coef, strip, strip_coef)


def lay_field(planes, cells, below, above, rows):
    for x, src, index, p in planes:
        if p is None:
            cells[0, x, PAD - EDGE : PAD + rows + EDGE] = src[index]
            continue
        cells[0, x, PAD : PAD + rows] = src[index]
        cells[0, x, PAD - WIDTH : PAD] = below(p)
        cells[0, x, PAD + rows : PAD + rows + WIDTH] = above(p)


def advance(out, cells, coef, strip, strip_coef):
    nx, rows = out.shape[:2]
    high = rows + 2 * EDGE
    shift = PAD - EDGE
    for step in range(1, WIDTH + 1):
        src, dst = (step - 1) % 2, step % 2
        last = step == WIDTH
        size = rows // 2 if last else high // 2
        for row in (EDGE, EDGE + size) if last else (0, size):
            here = shift + row
            lane = lax.broadcasted_iota(jnp.int32, (size, LANES), 1)
            start, end = lane == 0, lane == LANES - 1
            group, place = lane // WIDTH, lane % WIDTH
            low, top = (strip[src, side, here : here + size] for side in range(2))
            beyond = jnp.where(place == WIDTH - 1, low, pltpu.roll(top, WIDTH - 2, 1))
            inner = jnp.zeros((size, LANES), jnp.float32)
            before = cells[src, step - 1, here : here + size]
            mid = cells[src, step, here : here + size]
            for x in range(step, nx + 2 * WIDTH - step):
                after = cells[src, x + 1, here : here + size]
                turn = WIDTH * x + WIDTH - 1
                outer = pltpu.roll(beyond, (LANES - turn) % LANES, 1)
                if not last:
                    inner = jnp.where(group == x, pltpu.roll(mid, turn % LANES, 1), inner)
                c = [coef[k, x, row : row + size] for k in range(7)]
                new = c[0] * mid + c[1] * before + c[2] * after
                new += c[3] * cells[src, x, here - 1 : here - 1 + size]
                new += c[4] * cells[src, x, here + 1 : here + 1 + size]
                new += c[5] * jnp.where(start, outer, pltpu.roll(mid, 1, 1))
                new += c[6] * jnp.where(end, outer, pltpu.roll(mid, LANES - 1, 1))
                if last:
                    out[x - WIDTH, row - EDGE : row - EDGE + size] = new
                else:
                    cells[dst, x, here : here + size] = new
                before, mid = mid, after
            if last:
                continue
            for side in range(2):
                mid = low if side == 0 else top
                below, above = pltpu.roll(mid, 1, 1), pltpu.roll(mid, LANES - 1, 1)
                if side == 0:
                    above = jnp.where(place == WIDTH - 1, inner, above)
                else:
                    below = jnp.where(place == 0, pltpu.roll(inner, LANES - (WIDTH - 2), 1), below)
                c = [strip_coef[k, side, row : row + size] for k in range(7)]
                new = c[0] * mid + c[1] * pltpu.roll(mid, WIDTH, 1) + c[2] * pltpu.roll(mid, LANES - WIDTH, 1)
                new += c[3] * strip[src, side, here - 1 : here - 1 + size]
                new += c[4] * strip[src, side, here + 1 : here + 1 + size]
                new += c[5] * below + c[6] * above
                strip[dst, side, here : here + size] = new


def exchange_x(to_odd, to_even, shift, beside, args):
    count_x, count_y = lax.axis_size("gx"), lax.axis_size("gy")
    even = [(i, i + 1) for i in range(0, count_x, 2)]
    odd = [(i * count_y + j, (i + 1) * count_y + j) for i in range(1, count_x - 1, 2) for j in range(count_y)]
    odd += [(i * count_y + j, i * count_y + j + 1) for i in (0, count_x - 1) for j in range(0, count_y, 2)]

    def slide(k):
        pairs = []
        for j in range(count_y):
            top = (count_x - 1) * count_y + (j + k) % count_y
            pairs += [(j, top), (top, j)]
        return lambda a, *rest: (lax.ppermute(a, ("gx", "gy"), pairs), *beside(*rest))

    three = lax.ppermute(to_even, "gx", even + [(b, a) for a, b in even])
    one = lax.ppermute(to_odd, ("gx", "gy"), odd + [(b, a) for a, b in odd])
    slid, *rest = lax.switch(shift, [slide(k) for k in range(count_y)], to_odd, *args)
    return one, slid, three, rest


def shift_both(axis, up, down):
    n = lax.axis_size(axis)
    forth = [(i, (i + 1) % n) for i in range(n)]
    return lax.ppermute(up, axis, forth), lax.ppermute(down, axis, [(b, a) for a, b in forth])


def first_halo(inputs, to_odd, to_even, shift, place):
    total, rows, _ = to_odd.shape
    nx, count = inputs[0].shape[0], len(DEPTHS)
    high = rows + 2 * EDGE
    reach = rows // 2 + WIDTH

    def beside(*inputs):
        rim, lanes = (count * nx, WIDTH, LANES), (count, rows, LANES)
        own, up, down, z_up, z_down = call(prepare, [(count * nx, rows, LANES), rim, rim, lanes, lanes], inputs)
        return own, *shift_both("gy", up, down), z_up, z_down

    one, slid, three, (own, y_low, y_high, z_up, z_down) = exchange_x(to_odd, to_even, shift, beside, inputs)
    shape = (reach * total + WIDTH * total, LANES)
    up, down = call(functools.partial(pack_y, reach), [shape] * 2, [place, one, slid, three], (), 1)
    up, down, z_up, z_down = lax.optimization_barrier((up, down, z_up, z_down))
    ylo, yhi = shift_both("gy", up, down)
    z_up, z_down = call(pack_own_rims, [(count, high, LANES)] * 2, [y_low, y_high, z_up, z_down])
    z_low, z_high = shift_both("gz", z_up, z_down)
    sides, up, down = call(
        functools.partial(pack_sides, DEPTHS, reach),
        [(2 * total, high, LANES), (high, LANES), (high, LANES)],
        [place, one, slid, three, ylo, yhi],
        [(total, rows + 2 * reach, LANES)],
        1,
    )
    return own, [sides, y_low, y_high, z_low, z_high, *shift_both("gz", up, down)]


def second_halo(field, to_odd, to_even, shift, place):
    total, rows, _ = to_odd.shape
    nx = field.shape[0]
    reach = rows // 2 + WIDTH
    high = rows + 2 * EDGE
    one, slid, three, _ = exchange_x(to_odd, to_even, shift, lambda: (), [])
    shape = (reach * total + WIDTH * total + WIDTH * nx, LANES)
    up, down = call(functools.partial(pack_y, reach), [shape] * 2, [place, field, one, slid, three], (), 1)
    ylo, yhi = shift_both("gy", up, down)
    shape = (1, high, LANES)
    sides, up, down = call(
        functools.partial(pack_z, (WIDTH,), nx, reach),
        [(2 * total, high, LANES), shape, shape],
        [place, field, one, slid, three, ylo, yhi],
        [(total, rows + 2 * reach, LANES)],
        1,
    )
    return [sides, ylo, yhi, *shift_both("gz", up, down)]


def body(concentration, speed, signs, diffusivity, shear):
    nx, rows, lanes = concentration.shape
    count_x, count_y = lax.axis_size("gx"), lax.axis_size("gy")
    x_index = lax.axis_index("gx")
    blocks = (shear[0] + rows // 2) // rows
    shift, rest = blocks % count_y, shear[0] - blocks * rows
    crossed = (x_index == 0) | (x_index == count_x - 1)
    start = rows // 2 + jnp.where(x_index == 0, rest, -rest)
    odd = (x_index % 2).astype(jnp.int32).reshape(1)
    place = jnp.stack([x_index % 2, crossed.astype(jnp.int32), jnp.where(crossed, start, 0)]).astype(jnp.int32)
    face = (sum(DEPTHS), rows, lanes)
    inputs = [concentration, speed, signs, diffusivity]
    short = (2, WIDTH - 1, rows, lanes)
    to_odd, to_even = pl.pallas_call(
        first_faces,
        out_shape=[jax.ShapeDtypeStruct(face, jnp.float32)] * 2,
        in_specs=[SMEM] + [pl.BlockSpec(memory_space=pl.ANY)] * 4,
        out_specs=[VMEM] * 2,
        scratch_shapes=[
            pltpu.VMEM((2, WIDTH, rows, lanes), jnp.float32),
            pltpu.VMEM((2, 3, *short[1:]), jnp.float32),
            pltpu.VMEM((2, 3, *short[1:]), jnp.int32),
            pltpu.VMEM(short, jnp.float32),
            pltpu.SemaphoreType.DMA((8,)),
        ],
        compiler_params=pltpu.CompilerParams(vmem_limit_bytes=8 * 2**20),
    )(odd, *inputs)
    own, halo = first_halo(inputs, to_odd, to_even, shift, place)
    high = rows + 2 * EDGE
    wide = nx + 2 * WIDTH
    coef_shapes = [(7, wide, high, lanes), (7, 2, high, lanes)]
    scratch = [(2, wide, rows + 2 * PAD, lanes), (2, 2, rows + 2 * PAD, lanes)]
    face = (WIDTH, rows, lanes)
    field, to_odd, to_even, coef, strip_coef = call(
        first_steps, [(nx, rows, lanes), face, face, *coef_shapes], [odd, own, *halo], scratch, 1
    )
    later = second_halo(field, to_odd, to_even, shift, place)
    (field,) = call(last_steps, [(nx, rows, lanes)], [field, coef, strip_coef, *later], scratch)
    return field


def solution(mesh):
    placed = (
        P("gx", "gy", "gz"),
        P(None, "gx", "gy", "gz"),
        P(None, "gx", "gy", "gz"),
        P("gx", "gy", "gz"),
        P(),
    )
    return jax.shard_map(
        body, mesh=mesh, in_specs=placed, out_specs=P("gx", "gy", "gz"), check_vma=False
    )
```

```python
import functools
import math

import jax
import jax.numpy as jnp
from jax import lax
from jax.experimental import pallas as pl
from jax.experimental.pallas import tpu as pltpu
from jax.sharding import PartitionSpec as P

STEPS = 8
WIDTH = 4
TIME_STEP = 0.25
PAD = 16
EDGE = 8
LANES = 128

VMEM = pl.BlockSpec(memory_space=pltpu.VMEM)
SMEM = pl.BlockSpec(memory_space=pltpu.SMEM)
DEPTHS = (WIDTH, WIDTH - 1, WIDTH - 1, WIDTH - 1, WIDTH - 1)


def call(kernel, outs, args, scratch=(), scalars=0):
    need = sum(4 * math.prod(shape) for shape in list(outs) + list(scratch))
    need += sum(4 * math.prod(arg.shape) for arg in args[scalars:])
    return pl.pallas_call(
        kernel,
        out_shape=[jax.ShapeDtypeStruct(shape, jnp.float32) for shape in outs],
        in_specs=[SMEM] * scalars + [VMEM] * (len(args) - scalars),
        out_specs=[VMEM] * len(outs),
        scratch_shapes=[pltpu.VMEM(shape, jnp.float32) for shape in scratch],
        compiler_params=pltpu.CompilerParams(vmem_limit_bytes=need + 4 * 2**20),
    )(*args)


def first_faces(odd_ref, field, speed, signs, diffusivity, to_odd, to_slide, to_even, f, s, g, d, sems):
    nx = field.shape[0]
    copies = []
    for side in range(2):
        deep, short = (pl.ds(nx - n if side else 0, n) for n in DEPTHS[:2])
        for src, dst in (
            (field.at[deep], f.at[side]),
            (diffusivity.at[short], d.at[side]),
            (speed.at[:, short], s.at[side]),
            (signs.at[:, short], g.at[side]),
        ):
            copies.append(pltpu.make_async_copy(src, dst, sems.at[len(copies)]))
    for copy in copies:
        copy.start()
    for copy in copies:
        copy.wait()
    odd = odd_ref[0]
    for out, side in ((to_odd, odd), (to_even, 1 - odd)):
        for i in range(WIDTH):
            out[i] = f[side, i]
        for i in range(WIDTH - 1):
            out[WIDTH + i] = TIME_STEP * d[side, i]
            for k in range(3):
                scaled = TIME_STEP * s[side, k, i]
                out[WIDTH + (1 + k) * (WIDTH - 1) + i] = jnp.where(g[side, k, i] > 0, scaled, -scaled)
    for i in range(to_odd.shape[0]):
        to_slide[i] = to_odd[i]


def prepare(field, speed, signs, diffusivity, own, y_up, y_down, z_up, z_down):
    nx, rows = field.shape[:2]

    def plane(x, carry):
        own[x] = field[x]
        own[nx + x] = TIME_STEP * diffusivity[x]
        for d in range(3):
            scaled = TIME_STEP * speed[d, x]
            own[(2 + d) * nx + x] = jnp.where(signs[d, x] > 0, scaled, -scaled)
        return carry

    lax.fori_loop(0, nx, plane, 0)

    def edge(p, carry):
        y_up[p] = own[p, rows - WIDTH : rows, :]
        y_down[p] = own[p, 0:WIDTH, :]
        return carry

    lax.fori_loop(0, own.shape[0], edge, 0)

    def quantity(q, carry):
        for row in range(0, rows, 32):
            planes = [(WIDTH + i, own[q * nx + i, row : row + 32]) for i in range(nx)]
            up, down = pack_lanes(planes, 32)
            z_up[q, row : row + 32] = up
            z_down[q, row : row + 32] = down
        return carry

    lax.fori_loop(0, z_up.shape[0], quantity, 0)


def pack_lanes(planes, count):
    lane = lax.broadcasted_iota(jnp.int32, (count, LANES), 1)
    pair, lower = lane // (2 * WIDTH), lane % (2 * WIDTH) < WIDTH
    sums = [jnp.zeros((count, LANES), jnp.float32)] * 2
    for x, value in planes:
        m, k = x // 2, x % 2
        moved = pltpu.roll(value, (2 * WIDTH * m + WIDTH) % LANES, 1)
        sums[k] = jnp.where(pair == m, moved, sums[k])
    up = jnp.where(lower, sums[0], pltpu.roll(sums[1], WIDTH, 1))
    down = jnp.where(lower, pltpu.roll(sums[0], LANES - WIDTH, 1), sums[1])
    return up, down


def faces(odd, own, to_odd, to_slide, to_even, nx):
    a = jnp.where(odd > 0, nx - WIDTH, 0)
    b = jnp.where(odd > 0, 0, nx - WIDTH)
    for i in range(WIDTH):
        to_odd[i] = own[a + i]
        to_slide[i] = own[a + i]
        to_even[i] = own[b + i]


def pack_y(reach, place, *refs):
    *own, one, slid, three, up, down = refs
    crossed = place[1]
    rows, total = one.shape[1], one.shape[0]

    def wide(src):
        for i in range(total):
            up[reach * i : reach * (i + 1)] = src[i, rows - reach : rows, :]
            down[reach * i : reach * (i + 1)] = src[i, 0:reach, :]

    @pl.when(crossed > 0)
    def _():
        wide(slid)

    @pl.when(crossed == 0)
    def _():
        wide(one)

    at = reach * total
    for src in (three, *own):
        for i in range(src.shape[0]):
            up[at : at + WIDTH] = src[i, rows - WIDTH : rows, :]
            down[at : at + WIDTH] = src[i, 0:WIDTH, :]
            at += WIDTH


def planes_of(q, nx, depths, own, sides):
    depth, at, total = depths[q], sum(depths[:q]), sum(depths)
    low = [(WIDTH - depth + i, sides, at + i, None) for i in range(depth)]
    mid = [(WIDTH + i, own, q * nx + i, q * nx + i) for i in range(nx)]
    high = [(WIDTH + nx + i, sides, total + at + i, None) for i in range(depth)]
    return low + mid + high


def fetch(src, out, sem):
    copy = pltpu.make_async_copy(src, out, sem)
    copy.start()
    copy.wait()


def place_sides(reach, place, one, slid, three, ylo, yhi, sides, joined):
    rows, total = one.shape[1], one.shape[0]
    odd, crossed, start = place[0], place[1], place[2]

    def framed(src, base, i, below, above):
        at = base * total + i
        sides[at, EDGE : EDGE + rows] = src[i]
        sides[at, EDGE - WIDTH : EDGE] = ylo[below : below + WIDTH]
        sides[at, EDGE + rows : EDGE + rows + WIDTH] = yhi[above : above + WIDTH]

    for i in range(total):
        framed(three, 1 - odd, i, reach * total + WIDTH * i, reach * total + WIDTH * i)

    @pl.when(crossed > 0)
    def _():
        for i in range(total):
            joined[i, 0:reach] = ylo[reach * i : reach * (i + 1)]
            joined[i, reach : reach + rows] = slid[i]
            joined[i, reach + rows :] = yhi[reach * i : reach * (i + 1)]
        for i in range(total):
            sides[odd * total + i, EDGE - WIDTH : EDGE + rows + WIDTH] = joined[i, pl.ds(start, rows + 2 * WIDTH)]

    @pl.when(crossed == 0)
    def _():
        for i in range(total):
            framed(one, odd, i, reach * (i + 1) - WIDTH, reach * i)


def pack_own_rims(ylo, yhi, z_up, z_down, up, down):
    rows = z_up.shape[1]
    nx = ylo.shape[0] // z_up.shape[0]
    for q in range(z_up.shape[0]):
        for row, rim in ((EDGE - WIDTH, ylo), (EDGE + rows, yhi)):
            last, first = pack_lanes([(WIDTH + i, rim[q * nx + i]) for i in range(nx)], WIDTH)
            up[q, row : row + WIDTH] = last
            down[q, row : row + WIDTH] = first
        up[q, EDGE : EDGE + rows] = z_up[q]
        down[q, EDGE : EDGE + rows] = z_down[q]


def side_slots(depths):
    return [(2 * sum(depths[:q]), depth) for q, depth in enumerate(depths)]


def pack_sides(depths, reach, place, *refs):
    one, slid, three, ylo, yhi, sides, up, down, joined = refs
    place_sides(reach, place, one, slid, three, ylo, yhi, sides, joined)
    total = one.shape[0]
    for row in range(0, up.shape[0], 16):
        values = []
        for q, (slot, depth) in enumerate(side_slots(depths)):
            for i in range(depth):
                at = sum(depths[:q]) + i
                values.append((slot + i, sides[at, row : row + 16]))
                values.append((slot + depth + i, sides[total + at, row : row + 16]))
        up[row : row + 16], down[row : row + 16] = pack_lanes(values, 16)


def pack_z(depths, nx, reach, place, *refs):
    own, one, slid, three, ylo, yhi, sides, up, down, joined = refs
    place_sides(reach, place, one, slid, three, ylo, yhi, sides, joined)
    rows, total = one.shape[1], one.shape[0]
    later = WIDTH * total + reach * total
    for q in range(len(depths)):
        planes = planes_of(q, nx, depths, own, sides)
        for row, count in [(EDGE + r, 32) for r in range(0, rows, 32)] + [(EDGE - WIDTH, WIDTH), (EDGE + rows, WIDTH)]:
            values = []
            for x, src, index, p in planes:
                if p is None:
                    values.append((x, src[index, row : row + count]))
                elif count == WIDTH:
                    values.append((x, (ylo if row < EDGE else yhi)[later + WIDTH * p : later + WIDTH * (p + 1)]))
                else:
                    values.append((x, src[index, row - EDGE : row - EDGE + count]))
            up[q, row : row + count], down[q, row : row + count] = pack_lanes(values, count)


def derive(read, write):
    d = read(1)
    v = [read(2 + k) for k in range(3)]
    write(0, 1.0 - 6.0 * d - (v[0] + v[1] + v[2]))
    for k in range(3):
        write(1 + 2 * k, d + jnp.maximum(v[k], 0.0))
        write(2 + 2 * k, d + jnp.minimum(v[k], 0.0))


def advance(second, *refs):
    odd_ref, own = refs[0], refs[1]
    halo = refs[2:9]
    refs = refs[9:]
    if second:
        field_own, field_halo, depths = refs[0], refs[1:6], (WIDTH,)
        out = refs[6]
        refs = refs[7:]
    else:
        field_own, field_halo, depths = own, halo, DEPTHS
        out, to_odd, to_slide, to_even = refs[:4]
        refs = refs[4:]
    nx = out.shape[0]
    cells, coef, strip, strip_coef = refs
    rows = own.shape[1]
    high = rows + 2 * EDGE
    shift = PAD - EDGE

    for x, src, index, p in planes_of(0, nx, depths, field_own, field_halo[0]):
        if p is None:
            cells[0, x, shift : shift + high] = src[index]
            continue
        cells[0, x, PAD : PAD + rows] = src[index]
        at = field_halo[1].shape[0] - WIDTH * (nx - p)
        rim = (slice(at, at + WIDTH),) if second else (p,)
        cells[0, x, PAD - WIDTH : PAD] = field_halo[1][rim]
        cells[0, x, PAD + rows : PAD + rows + WIDTH] = field_halo[2][rim]
    lane = lax.broadcasted_iota(jnp.int32, (high, LANES), 1)
    inside = (lane >= WIDTH * WIDTH) & (lane < WIDTH * (WIDTH + nx))
    slots = side_slots(DEPTHS)

    def z_halo(q, side):
        slot, depth = slots[q]
        packed = halo[5 + side][...]
        low = pltpu.roll(packed, WIDTH * (WIDTH - depth - slot) % LANES, 1)
        top = pltpu.roll(packed, WIDTH * (WIDTH + nx - slot - depth) % LANES, 1)
        return jnp.where(inside, halo[3 + side][q], jnp.where(lane < WIDTH * WIDTH, low, top))

    for side in range(2):
        strip[0, side, shift : shift + high] = field_halo[3 + side][0] if second else z_halo(0, side)

        def write(k, value, side=side):
            strip_coef[k, side] = value

        derive(functools.partial(z_halo, side=side), write)
    for four in zip(*[planes_of(q, nx, DEPTHS, own, halo[0]) for q in range(1, 5)]):
        x, p = four[0][0], four[0][3]

        def at(row, count, x=x):
            def write(k, value):
                coef[k, x, row : row + count] = value

            return write

        offset = 0 if p is None else EDGE
        for r in range(0, high if p is None else rows, 16):
            derive(lambda q, r=r, four=four: four[q - 1][1][four[q - 1][2], r : r + 16], at(offset + r, 16))
        if p is not None:
            derive(lambda q, four=four: halo[1][four[q - 1][3]], at(EDGE - WIDTH, WIDTH))
            derive(lambda q, four=four: halo[2][four[q - 1][3]], at(EDGE + rows, WIDTH))

    for step in range(1, WIDTH + 1):
        src, dst = (step - 1) % 2, step % 2
        last = step == WIDTH
        size = rows // 2 if last else high // 2
        for row in (EDGE, EDGE + size) if last else (0, size):
            here = shift + row
            lane = lax.broadcasted_iota(jnp.int32, (size, LANES), 1)
            start, end = lane == 0, lane == LANES - 1
            group, place = lane // WIDTH, lane % WIDTH
            low, top = (strip[src, side, here : here + size] for side in range(2))
            beyond = jnp.where(place == WIDTH - 1, low, pltpu.roll(top, WIDTH - 2, 1))
            inner = jnp.zeros((size, LANES), jnp.float32)
            before = cells[src, step - 1, here : here + size]
            mid = cells[src, step, here : here + size]
            for x in range(step, nx + 2 * WIDTH - step):
                after = cells[src, x + 1, here : here + size]
                turn = WIDTH * x + WIDTH - 1
                outer = pltpu.roll(beyond, (LANES - turn) % LANES, 1)
                if not last:
                    inner = jnp.where(group == x, pltpu.roll(mid, turn % LANES, 1), inner)
                c = [coef[k, x, row : row + size] for k in range(7)]
                new = c[0] * mid + c[1] * before + c[2] * after
                new += c[3] * cells[src, x, here - 1 : here - 1 + size]
                new += c[4] * cells[src, x, here + 1 : here + 1 + size]
                new += c[5] * jnp.where(start, outer, pltpu.roll(mid, 1, 1))
                new += c[6] * jnp.where(end, outer, pltpu.roll(mid, LANES - 1, 1))
                if last:
                    out[x - WIDTH, row - EDGE : row - EDGE + size] = new
                else:
                    cells[dst, x, here : here + size] = new
                before, mid = mid, after
            if last:
                continue
            for side in range(2):
                mid = low if side == 0 else top
                below, above = pltpu.roll(mid, 1, 1), pltpu.roll(mid, LANES - 1, 1)
                if side == 0:
                    above = jnp.where(place == WIDTH - 1, inner, above)
                else:
                    below = jnp.where(place == 0, pltpu.roll(inner, LANES - (WIDTH - 2), 1), below)
                c = [strip_coef[k, side, row : row + size] for k in range(7)]
                new = c[0] * mid + c[1] * pltpu.roll(mid, WIDTH, 1) + c[2] * pltpu.roll(mid, LANES - WIDTH, 1)
                new += c[3] * strip[src, side, here - 1 : here - 1 + size]
                new += c[4] * strip[src, side, here + 1 : here + 1 + size]
                new += c[5] * below + c[6] * above
                strip[dst, side, here : here + size] = new
    if not second:
        faces(odd_ref[0], out, to_odd, to_slide, to_even, nx)


def exchange_x(to_odd, to_slide, to_even, shift, beside, args):
    count_x, count_y = lax.axis_size("gx"), lax.axis_size("gy")
    even = [(i, i + 1) for i in range(0, count_x, 2)]
    odd = [(i * count_y + j, (i + 1) * count_y + j) for i in range(1, count_x - 1, 2) for j in range(count_y)]
    odd += [(i * count_y + j, i * count_y + j + 1) for i in (0, count_x - 1) for j in range(0, count_y, 2)]

    def slide(k):
        pairs = []
        for j in range(count_y):
            top = (count_x - 1) * count_y + (j + k) % count_y
            pairs += [(j, top), (top, j)]
        return lambda a, *rest: (lax.ppermute(a, ("gx", "gy"), pairs), *beside(*rest))

    three = lax.ppermute(to_even, "gx", even + [(b, a) for a, b in even])
    one = lax.ppermute(to_odd, ("gx", "gy"), odd + [(b, a) for a, b in odd])
    slid, *rest = lax.switch(shift, [slide(k) for k in range(count_y)], to_slide, *args)
    return one, slid, three, rest


def shift_both(axis, up, down):
    n = lax.axis_size(axis)
    forth = [(i, (i + 1) % n) for i in range(n)]
    return lax.ppermute(up, axis, forth), lax.ppermute(down, axis, [(b, a) for a, b in forth])


def first_halo(inputs, to_odd, to_slide, to_even, shift, place):
    total, rows, _ = to_odd.shape
    nx, count = inputs[0].shape[0], len(DEPTHS)
    high = rows + 2 * EDGE
    reach = rows // 2 + WIDTH

    def beside(*inputs):
        rim, lanes = (count * nx, WIDTH, LANES), (count, rows, LANES)
        own, up, down, z_up, z_down = call(prepare, [(count * nx, rows, LANES), rim, rim, lanes, lanes], inputs)
        return own, *shift_both("gy", up, down), z_up, z_down

    one, slid, three, (own, y_low, y_high, z_up, z_down) = exchange_x(to_odd, to_slide, to_even, shift, beside, inputs)
    shape = (reach * total + WIDTH * total, LANES)
    up, down = call(functools.partial(pack_y, reach), [shape] * 2, [place, one, slid, three], (), 1)
    up, down, z_up, z_down = lax.optimization_barrier((up, down, z_up, z_down))
    ylo, yhi = shift_both("gy", up, down)
    z_up, z_down = call(pack_own_rims, [(count, high, LANES)] * 2, [y_low, y_high, z_up, z_down])
    z_low, z_high = shift_both("gz", z_up, z_down)
    sides, up, down = call(
        functools.partial(pack_sides, DEPTHS, reach),
        [(2 * total, high, LANES), (high, LANES), (high, LANES)],
        [place, one, slid, three, ylo, yhi],
        [(total, rows + 2 * reach, LANES)],
        1,
    )
    return own, [sides, y_low, y_high, z_low, z_high, *shift_both("gz", up, down)]


def second_halo(field, own, to_odd, to_slide, to_even, shift, place):
    total, rows, _ = to_odd.shape
    nx = field.shape[0]
    reach = rows // 2 + WIDTH
    high = rows + 2 * EDGE
    one, slid, three, _ = exchange_x(to_odd, to_slide, to_even, shift, lambda: (), [])
    shape = (reach * total + WIDTH * total + WIDTH * nx, LANES)
    up, down = call(functools.partial(pack_y, reach), [shape] * 2, [place, field, one, slid, three], (), 1)
    up, down, own = lax.optimization_barrier((up, down, own))
    ylo, yhi = shift_both("gy", up, down)
    own = pl.pallas_call(
        fetch,
        out_shape=jax.ShapeDtypeStruct(own.shape, own.dtype),
        in_specs=[pl.BlockSpec(memory_space=pl.ANY)],
        out_specs=VMEM,
        scratch_shapes=[pltpu.SemaphoreType.DMA(())],
        compiler_params=pltpu.CompilerParams(vmem_limit_bytes=4 * 2**20),
    )(own)
    shape = (1, high, LANES)
    sides, up, down = call(
        functools.partial(pack_z, (WIDTH,), nx, reach),
        [(2 * total, high, LANES), shape, shape],
        [place, field, one, slid, three, ylo, yhi],
        [(total, rows + 2 * reach, LANES)],
        1,
    )
    return own, [sides, ylo, yhi, *shift_both("gz", up, down)]


def body(concentration, speed, signs, diffusivity, shear):
    nx, rows, lanes = concentration.shape
    count_x, count_y = lax.axis_size("gx"), lax.axis_size("gy")
    x_index = lax.axis_index("gx")
    blocks = (shear[0] + rows // 2) // rows
    shift, rest = blocks % count_y, shear[0] - blocks * rows
    crossed = (x_index == 0) | (x_index == count_x - 1)
    start = rows // 2 + jnp.where(x_index == 0, rest, -rest)
    odd = (x_index % 2).astype(jnp.int32).reshape(1)
    place = jnp.stack([x_index % 2, crossed.astype(jnp.int32), jnp.where(crossed, start, 0)]).astype(jnp.int32)
    face = (sum(DEPTHS), rows, lanes)
    inputs = [concentration, speed, signs, diffusivity]
    short = (2, WIDTH - 1, rows, lanes)
    to_odd, to_slide, to_even = pl.pallas_call(
        first_faces,
        out_shape=[jax.ShapeDtypeStruct(face, jnp.float32)] * 3,
        in_specs=[SMEM] + [pl.BlockSpec(memory_space=pl.ANY)] * 4,
        out_specs=[VMEM] * 3,
        scratch_shapes=[
            pltpu.VMEM((2, WIDTH, rows, lanes), jnp.float32),
            pltpu.VMEM((2, 3, *short[1:]), jnp.float32),
            pltpu.VMEM((2, 3, *short[1:]), jnp.int32),
            pltpu.VMEM(short, jnp.float32),
            pltpu.SemaphoreType.DMA((8,)),
        ],
        compiler_params=pltpu.CompilerParams(vmem_limit_bytes=8 * 2**20),
    )(odd, *inputs)
    own, halo = first_halo(inputs, to_odd, to_slide, to_even, shift, place)
    high = rows + 2 * EDGE
    wide = nx + 2 * WIDTH
    scratch = [(2, wide, rows + 2 * PAD, lanes), (7, wide, high, lanes), (2, 2, rows + 2 * PAD, lanes), (7, 2, high, lanes)]
    face = (WIDTH, rows, lanes)
    field, to_odd, to_slide, to_even = call(
        functools.partial(advance, False), [(nx, rows, lanes), face, face, face], [odd, own, *halo], scratch, 1
    )
    own, later = second_halo(field, own, to_odd, to_slide, to_even, shift, place)
    (field,) = call(
        functools.partial(advance, True), [(nx, rows, lanes)], [odd, own, *halo, field, *later], scratch, 1
    )
    return field


def solution(mesh):
    placed = (
        P("gx", "gy", "gz"),
        P(None, "gx", "gy", "gz"),
        P(None, "gx", "gy", "gz"),
        P("gx", "gy", "gz"),
        P(),
    )
    return jax.shard_map(
        body, mesh=mesh, in_specs=placed, out_specs=P("gx", "gy", "gz"), check_vma=False
    )
```

```python
import functools
import math

import jax
import jax.numpy as jnp
from jax import lax
from jax.experimental import pallas as pl
from jax.experimental.pallas import tpu as pltpu
from jax.sharding import PartitionSpec as P


WIDTH = 4
TIME_STEP = 0.25
PAD = 16
EDGE = 8
LANES = 128

VMEM = pl.BlockSpec(memory_space=pltpu.VMEM)
SMEM = pl.BlockSpec(memory_space=pltpu.SMEM)
DEPTHS = (WIDTH, WIDTH - 1, WIDTH - 1, WIDTH - 1, WIDTH - 1)


def call(kernel, outs, args, scratch=(), scalars=0):
    need = sum(4 * math.prod(shape) for shape in list(outs) + list(scratch))
    need += sum(4 * math.prod(arg.shape) for arg in args[scalars:])
    return pl.pallas_call(
        kernel,
        out_shape=[jax.ShapeDtypeStruct(shape, jnp.float32) for shape in outs],
        in_specs=[SMEM] * scalars + [VMEM] * (len(args) - scalars),
        out_specs=[VMEM] * len(outs),
        scratch_shapes=[pltpu.VMEM(shape, jnp.float32) for shape in scratch],
        compiler_params=pltpu.CompilerParams(vmem_limit_bytes=need + 4 * 2**20),
    )(*args)


def first_faces(odd_ref, field, speed, signs, diffusivity, to_odd, to_slide, to_even, f, s, g, d, sems):
    nx = field.shape[0]
    copies = []
    for side in range(2):
        deep, short = (pl.ds(nx - n if side else 0, n) for n in DEPTHS[:2])
        for src, dst in (
            (field.at[deep], f.at[side]),
            (diffusivity.at[short], d.at[side]),
            (speed.at[:, short], s.at[side]),
            (signs.at[:, short], g.at[side]),
        ):
            copies.append(pltpu.make_async_copy(src, dst, sems.at[len(copies)]))
    for copy in copies:
        copy.start()
    for copy in copies:
        copy.wait()
    odd = odd_ref[0]
    for out, side in ((to_odd, odd), (to_even, 1 - odd)):
        for i in range(WIDTH):
            out[i] = f[side, i]
        for i in range(WIDTH - 1):
            out[WIDTH + i] = TIME_STEP * d[side, i]
            for k in range(3):
                scaled = TIME_STEP * s[side, k, i]
                out[WIDTH + (1 + k) * (WIDTH - 1) + i] = jnp.where(g[side, k, i] > 0, scaled, -scaled)
    for i in range(to_odd.shape[0]):
        to_slide[i] = to_odd[i]


def prepare(field, speed, signs, diffusivity, own, y_up, y_down, z_up, z_down):
    nx, rows = field.shape[:2]

    def plane(x, carry):
        own[x] = field[x]
        own[nx + x] = TIME_STEP * diffusivity[x]
        for d in range(3):
            scaled = TIME_STEP * speed[d, x]
            own[(2 + d) * nx + x] = jnp.where(signs[d, x] > 0, scaled, -scaled)
        return carry

    lax.fori_loop(0, nx, plane, 0)

    def edge(p, carry):
        y_up[p] = own[p, rows - WIDTH : rows, :]
        y_down[p] = own[p, 0:WIDTH, :]
        return carry

    lax.fori_loop(0, own.shape[0], edge, 0)

    def quantity(q, carry):
        for row in range(0, rows, 32):
            planes = [(WIDTH + i, own[q * nx + i, row : row + 32]) for i in range(nx)]
            up, down = pack_lanes(planes, 32)
            z_up[q, row : row + 32] = up
            z_down[q, row : row + 32] = down
        return carry

    lax.fori_loop(0, z_up.shape[0], quantity, 0)


def pack_lanes(planes, count):
    lane = lax.broadcasted_iota(jnp.int32, (count, LANES), 1)
    pair, lower = lane // (2 * WIDTH), lane % (2 * WIDTH) < WIDTH
    sums = [jnp.zeros((count, LANES), jnp.float32)] * 2
    for x, value in planes:
        m, k = x // 2, x % 2
        moved = pltpu.roll(value, (2 * WIDTH * m + WIDTH) % LANES, 1)
        sums[k] = jnp.where(pair == m, moved, sums[k])
    up = jnp.where(lower, sums[0], pltpu.roll(sums[1], WIDTH, 1))
    down = jnp.where(lower, pltpu.roll(sums[0], LANES - WIDTH, 1), sums[1])
    return up, down


def faces(odd, own, to_odd, to_slide, to_even, nx):
    a = jnp.where(odd > 0, nx - WIDTH, 0)
    b = jnp.where(odd > 0, 0, nx - WIDTH)
    for i in range(WIDTH):
        to_odd[i] = own[a + i]
        to_slide[i] = own[a + i]
        to_even[i] = own[b + i]


def pack_y(reach, place, *refs):
    *own, one, slid, three, up, down, held = refs
    crossed = place[1]
    rows, total = one.shape[1], one.shape[0]

    def wide(src):
        for i in range(total):
            up[reach * i : reach * (i + 1)] = src[i, rows - reach : rows, :]
            down[reach * i : reach * (i + 1)] = src[i, 0:reach, :]

    @pl.when(crossed > 0)
    def _():
        wide(slid)
        for i in range(total):
            held[i] = slid[i]

    @pl.when(crossed == 0)
    def _():
        wide(one)

    at = reach * total
    for src in (three, *own):
        for i in range(src.shape[0]):
            up[at : at + WIDTH] = src[i, rows - WIDTH : rows, :]
            down[at : at + WIDTH] = src[i, 0:WIDTH, :]
            at += WIDTH


def planes_of(q, nx, depths, own, sides):
    depth, at, total = depths[q], sum(depths[:q]), sum(depths)
    low = [(WIDTH - depth + i, sides, at + i, None) for i in range(depth)]
    mid = [(WIDTH + i, own, q * nx + i, q * nx + i) for i in range(nx)]
    high = [(WIDTH + nx + i, sides, total + at + i, None) for i in range(depth)]
    return low + mid + high


def fetch(src, out, sem):
    copy = pltpu.make_async_copy(src, out, sem)
    copy.start()
    copy.wait()


def place_sides(reach, place, one, slid, three, ylo, yhi, sides, joined):
    rows, total = one.shape[1], one.shape[0]
    odd, crossed, start = place[0], place[1], place[2]

    def framed(src, base, i, below, above):
        at = base * total + i
        sides[at, EDGE : EDGE + rows] = src[i]
        sides[at, EDGE - WIDTH : EDGE] = ylo[below : below + WIDTH]
        sides[at, EDGE + rows : EDGE + rows + WIDTH] = yhi[above : above + WIDTH]

    for i in range(total):
        framed(three, 1 - odd, i, reach * total + WIDTH * i, reach * total + WIDTH * i)

    @pl.when(crossed > 0)
    def _():
        for i in range(total):
            joined[i, 0:reach] = ylo[reach * i : reach * (i + 1)]
            joined[i, reach : reach + rows] = slid[i]
            joined[i, reach + rows :] = yhi[reach * i : reach * (i + 1)]
        for i in range(total):
            sides[odd * total + i, EDGE - WIDTH : EDGE + rows + WIDTH] = joined[i, pl.ds(start, rows + 2 * WIDTH)]

    @pl.when(crossed == 0)
    def _():
        for i in range(total):
            framed(one, odd, i, reach * (i + 1) - WIDTH, reach * i)


def pack_own_rims(ylo, yhi, z_up, z_down, up, down, low, high):
    rows = z_up.shape[1]
    nx = ylo.shape[0] // z_up.shape[0]
    for q in range(z_up.shape[0]):
        for row, rim in ((EDGE - WIDTH, ylo), (EDGE + rows, yhi)):
            last, first = pack_lanes([(WIDTH + i, rim[q * nx + i]) for i in range(nx)], WIDTH)
            up[q, row : row + WIDTH] = last
            down[q, row : row + WIDTH] = first
        up[q, EDGE : EDGE + rows] = z_up[q]
        down[q, EDGE : EDGE + rows] = z_down[q]

    def rim(p, carry):
        low[p] = ylo[p]
        high[p] = yhi[p]
        return carry

    lax.fori_loop(0, ylo.shape[0], rim, 0)


def side_slots(depths):
    return [(2 * sum(depths[:q]), depth) for q, depth in enumerate(depths)]


def pack_sides(depths, reach, place, *refs):
    one, slid, three, ylo, yhi, sides, up, down, joined = refs
    place_sides(reach, place, one, slid, three, ylo, yhi, sides, joined)
    total = one.shape[0]
    for row in range(0, up.shape[0], 16):
        values = []
        for q, (slot, depth) in enumerate(side_slots(depths)):
            for i in range(depth):
                at = sum(depths[:q]) + i
                values.append((slot + i, sides[at, row : row + 16]))
                values.append((slot + depth + i, sides[total + at, row : row + 16]))
        up[row : row + 16], down[row : row + 16] = pack_lanes(values, 16)


def pack_z(depths, nx, reach, place, *refs):
    own, one, slid, three, ylo, yhi, sides, up, down, joined = refs
    place_sides(reach, place, one, slid, three, ylo, yhi, sides, joined)
    rows, total = one.shape[1], one.shape[0]
    later = WIDTH * total + reach * total
    for q in range(len(depths)):
        planes = planes_of(q, nx, depths, own, sides)
        for row, count in [(EDGE + r, 32) for r in range(0, rows, 32)] + [(EDGE - WIDTH, WIDTH), (EDGE + rows, WIDTH)]:
            values = []
            for x, src, index, p in planes:
                if p is None:
                    values.append((x, src[index, row : row + count]))
                elif count == WIDTH:
                    values.append((x, (ylo if row < EDGE else yhi)[later + WIDTH * p : later + WIDTH * (p + 1)]))
                else:
                    values.append((x, src[index, row - EDGE : row - EDGE + count]))
            up[q, row : row + count], down[q, row : row + count] = pack_lanes(values, count)


def derive(read, write):
    d = read(1)
    v = [read(2 + k) for k in range(3)]
    write(0, 1.0 - 6.0 * d - (v[0] + v[1] + v[2]))
    for k in range(3):
        write(1 + 2 * k, d + jnp.maximum(v[k], 0.0))
        write(2 + 2 * k, d + jnp.minimum(v[k], 0.0))


def advance(second, *refs):
    odd_ref, own = refs[0], refs[1]
    halo = refs[2:9]
    refs = refs[9:]
    if second:
        field_own, field_halo, depths = refs[0], refs[1:6], (WIDTH,)
        out = refs[6]
        refs = refs[7:]
    else:
        field_own, field_halo, depths = own, halo, DEPTHS
        out, to_odd, to_slide, to_even = refs[:4]
        refs = refs[4:]
    nx = out.shape[0]
    cells, coef, strip, strip_coef = refs
    rows = own.shape[1]
    high = rows + 2 * EDGE
    shift = PAD - EDGE

    for x, src, index, p in planes_of(0, nx, depths, field_own, field_halo[0]):
        if p is None:
            cells[0, x, shift : shift + high] = src[index]
            continue
        cells[0, x, PAD : PAD + rows] = src[index]
        at = field_halo[1].shape[0] - WIDTH * (nx - p)
        rim = (slice(at, at + WIDTH),) if second else (p,)
        cells[0, x, PAD - WIDTH : PAD] = field_halo[1][rim]
        cells[0, x, PAD + rows : PAD + rows + WIDTH] = field_halo[2][rim]
    lane = lax.broadcasted_iota(jnp.int32, (high, LANES), 1)
    inside = (lane >= WIDTH * WIDTH) & (lane < WIDTH * (WIDTH + nx))
    slots = side_slots(DEPTHS)

    def z_halo(q, side):
        slot, depth = slots[q]
        packed = halo[5 + side][...]
        low = pltpu.roll(packed, WIDTH * (WIDTH - depth - slot) % LANES, 1)
        top = pltpu.roll(packed, WIDTH * (WIDTH + nx - slot - depth) % LANES, 1)
        return jnp.where(inside, halo[3 + side][q], jnp.where(lane < WIDTH * WIDTH, low, top))

    for side in range(2):
        strip[0, side, shift : shift + high] = field_halo[3 + side][0] if second else z_halo(0, side)

        def write(k, value, side=side):
            strip_coef[k, side] = value

        derive(functools.partial(z_halo, side=side), write)
    for four in zip(*[planes_of(q, nx, DEPTHS, own, halo[0]) for q in range(1, 5)]):
        x, p = four[0][0], four[0][3]

        def at(row, count, x=x):
            def write(k, value):
                coef[k, x, row : row + count] = value

            return write

        offset = 0 if p is None else EDGE
        for r in range(0, high if p is None else rows, 16):
            derive(lambda q, r=r, four=four: four[q - 1][1][four[q - 1][2], r : r + 16], at(offset + r, 16))
        if p is not None:
            derive(lambda q, four=four: halo[1][four[q - 1][3]], at(EDGE - WIDTH, WIDTH))
            derive(lambda q, four=four: halo[2][four[q - 1][3]], at(EDGE + rows, WIDTH))

    for step in range(1, WIDTH + 1):
        src, dst = (step - 1) % 2, step % 2
        last = step == WIDTH
        size = rows // 2 if last else high // 2
        for row in (EDGE, EDGE + size) if last else (0, size):
            here = shift + row
            lane = lax.broadcasted_iota(jnp.int32, (size, LANES), 1)
            start, end = lane == 0, lane == LANES - 1
            group, place = lane // WIDTH, lane % WIDTH
            low, top = (strip[src, side, here : here + size] for side in range(2))
            beyond = jnp.where(place == WIDTH - 1, low, pltpu.roll(top, WIDTH - 2, 1))
            inner = jnp.zeros((size, LANES), jnp.float32)
            before = cells[src, step - 1, here : here + size]
            mid = cells[src, step, here : here + size]
            for x in range(step, nx + 2 * WIDTH - step):
                after = cells[src, x + 1, here : here + size]
                turn = WIDTH * x + WIDTH - 1
                outer = pltpu.roll(beyond, (LANES - turn) % LANES, 1)
                if not last:
                    inner = jnp.where(group == x, pltpu.roll(mid, turn % LANES, 1), inner)
                c = [coef[k, x, row : row + size] for k in range(7)]
                new = c[0] * mid + c[1] * before + c[2] * after
                new += c[3] * cells[src, x, here - 1 : here - 1 + size]
                new += c[4] * cells[src, x, here + 1 : here + 1 + size]
                new += c[5] * jnp.where(start, outer, pltpu.roll(mid, 1, 1))
                new += c[6] * jnp.where(end, outer, pltpu.roll(mid, LANES - 1, 1))
                if last:
                    out[x - WIDTH, row - EDGE : row - EDGE + size] = new
                else:
                    cells[dst, x, here : here + size] = new
                before, mid = mid, after
            if last:
                continue
            for side in range(2):
                mid = low if side == 0 else top
                below, above = pltpu.roll(mid, 1, 1), pltpu.roll(mid, LANES - 1, 1)
                if side == 0:
                    above = jnp.where(place == WIDTH - 1, inner, above)
                else:
                    below = jnp.where(place == 0, pltpu.roll(inner, LANES - (WIDTH - 2), 1), below)
                c = [strip_coef[k, side, row : row + size] for k in range(7)]
                new = c[0] * mid + c[1] * pltpu.roll(mid, WIDTH, 1) + c[2] * pltpu.roll(mid, LANES - WIDTH, 1)
                new += c[3] * strip[src, side, here - 1 : here - 1 + size]
                new += c[4] * strip[src, side, here + 1 : here + 1 + size]
                new += c[5] * below + c[6] * above
                strip[dst, side, here : here + size] = new
    if not second:
        faces(odd_ref[0], out, to_odd, to_slide, to_even, nx)


def exchange_x(to_odd, to_slide, to_even, shift, beside, args):
    count_x, count_y = lax.axis_size("gx"), lax.axis_size("gy")
    even = [(i, i + 1) for i in range(0, count_x, 2)]
    odd = [(i * count_y + j, (i + 1) * count_y + j) for i in range(1, count_x - 1, 2) for j in range(count_y)]
    odd += [(i * count_y + j, i * count_y + j + 1) for i in (0, count_x - 1) for j in range(0, count_y, 2)]

    def slide(k):
        pairs = []
        for j in range(count_y):
            top = (count_x - 1) * count_y + (j + k) % count_y
            pairs += [(j, top), (top, j)]
        return lambda a, *rest: (lax.ppermute(a, ("gx", "gy"), pairs), *beside(*rest))

    three = lax.ppermute(to_even, "gx", even + [(b, a) for a, b in even])
    one = lax.ppermute(to_odd, ("gx", "gy"), odd + [(b, a) for a, b in odd])
    slid, *rest = lax.switch(shift, [slide(k) for k in range(count_y)], to_slide, *args)
    return one, slid, three, rest


def shift_both(axis, up, down):
    n = lax.axis_size(axis)
    forth = [(i, (i + 1) % n) for i in range(n)]
    return lax.ppermute(up, axis, forth), lax.ppermute(down, axis, [(b, a) for a, b in forth])


def first_halo(inputs, to_odd, to_slide, to_even, shift, place):
    total, rows, _ = to_odd.shape
    nx, count = inputs[0].shape[0], len(DEPTHS)
    high = rows + 2 * EDGE
    reach = rows // 2 + WIDTH

    def beside(*inputs):
        rim, lanes = (count * nx, WIDTH, LANES), (count, rows, LANES)
        own, up, down, z_up, z_down = call(prepare, [(count * nx, rows, LANES), rim, rim, lanes, lanes], inputs)
        return own, *shift_both("gy", up, down), z_up, z_down

    one, slid, three, (own, y_low, y_high, z_up, z_down) = exchange_x(to_odd, to_slide, to_even, shift, beside, inputs)
    shape = (reach * total + WIDTH * total, LANES)
    up, down, slid = call(functools.partial(pack_y, reach), [shape] * 2 + [slid.shape], [place, one, slid, three], (), 1)
    up, down, z_up, z_down = lax.optimization_barrier((up, down, z_up, z_down))
    ylo, yhi = shift_both("gy", up, down)
    shapes = [(count, high, LANES)] * 2 + [y_low.shape] * 2
    z_up, z_down, y_low, y_high = call(pack_own_rims, shapes, [y_low, y_high, z_up, z_down])
    z_low, z_high = shift_both("gz", z_up, z_down)
    sides, up, down = call(
        functools.partial(pack_sides, DEPTHS, reach),
        [(2 * total, high, LANES), (high, LANES), (high, LANES)],
        [place, one, slid, three, ylo, yhi],
        [(total, rows + 2 * reach, LANES)],
        1,
    )
    return own, [sides, y_low, y_high, z_low, z_high, *shift_both("gz", up, down)]


def second_halo(field, own, to_odd, to_slide, to_even, shift, place):
    total, rows, _ = to_odd.shape
    nx = field.shape[0]
    reach = rows // 2 + WIDTH
    high = rows + 2 * EDGE
    one, slid, three, _ = exchange_x(to_odd, to_slide, to_even, shift, lambda: (), [])
    shape = (reach * total + WIDTH * total + WIDTH * nx, LANES)
    args = [place, field, one, slid, three]
    up, down, slid = call(functools.partial(pack_y, reach), [shape] * 2 + [slid.shape], args, (), 1)
    up, down, own = lax.optimization_barrier((up, down, own))
    ylo, yhi = shift_both("gy", up, down)
    own = pl.pallas_call(
        fetch,
        out_shape=jax.ShapeDtypeStruct(own.shape, own.dtype),
        in_specs=[pl.BlockSpec(memory_space=pl.ANY)],
        out_specs=VMEM,
        scratch_shapes=[pltpu.SemaphoreType.DMA(())],
        compiler_params=pltpu.CompilerParams(vmem_limit_bytes=4 * 2**20),
    )(own)
    shape = (1, high, LANES)
    sides, up, down = call(
        functools.partial(pack_z, (WIDTH,), nx, reach),
        [(2 * total, high, LANES), shape, shape],
        [place, field, one, slid, three, ylo, yhi],
        [(total, rows + 2 * reach, LANES)],
        1,
    )
    return own, [sides, ylo, yhi, *shift_both("gz", up, down)]


def body(concentration, speed, signs, diffusivity, shear):
    nx, rows, lanes = concentration.shape
    count_x, count_y = lax.axis_size("gx"), lax.axis_size("gy")
    x_index = lax.axis_index("gx")
    blocks = (shear[0] + rows // 2) // rows
    shift, rest = blocks % count_y, shear[0] - blocks * rows
    crossed = (x_index == 0) | (x_index == count_x - 1)
    start = rows // 2 + jnp.where(x_index == 0, rest, -rest)
    odd = (x_index % 2).astype(jnp.int32).reshape(1)
    place = jnp.stack([x_index % 2, crossed.astype(jnp.int32), jnp.where(crossed, start, 0)]).astype(jnp.int32)
    face = (sum(DEPTHS), rows, lanes)
    inputs = [concentration, speed, signs, diffusivity]
    short = (2, WIDTH - 1, rows, lanes)
    to_odd, to_slide, to_even = pl.pallas_call(
        first_faces,
        out_shape=[jax.ShapeDtypeStruct(face, jnp.float32)] * 3,
        in_specs=[SMEM] + [pl.BlockSpec(memory_space=pl.ANY)] * 4,
        out_specs=[VMEM] * 3,
        scratch_shapes=[
            pltpu.VMEM((2, WIDTH, rows, lanes), jnp.float32),
            pltpu.VMEM((2, 3, *short[1:]), jnp.float32),
            pltpu.VMEM((2, 3, *short[1:]), jnp.int32),
            pltpu.VMEM(short, jnp.float32),
            pltpu.SemaphoreType.DMA((8,)),
        ],
        compiler_params=pltpu.CompilerParams(vmem_limit_bytes=8 * 2**20),
    )(odd, *inputs)
    own, halo = first_halo(inputs, to_odd, to_slide, to_even, shift, place)
    high = rows + 2 * EDGE
    wide = nx + 2 * WIDTH
    scratch = [(2, wide, rows + 2 * PAD, lanes), (7, wide, high, lanes), (2, 2, rows + 2 * PAD, lanes), (7, 2, high, lanes)]
    face = (WIDTH, rows, lanes)
    field, to_odd, to_slide, to_even = call(
        functools.partial(advance, False), [(nx, rows, lanes), face, face, face], [odd, own, *halo], scratch, 1
    )
    own, later = second_halo(field, own, to_odd, to_slide, to_even, shift, place)
    (field,) = call(
        functools.partial(advance, True), [(nx, rows, lanes)], [odd, own, *halo, field, *later], scratch, 1
    )
    return field


def solution(mesh):
    placed = (
        P("gx", "gy", "gz"),
        P(None, "gx", "gy", "gz"),
        P(None, "gx", "gy", "gz"),
        P("gx", "gy", "gz"),
        P(),
    )

    return jax.shard_map(body, mesh=mesh, in_specs=placed, out_specs=P("gx", "gy", "gz"), check_vma=False)
```

```python
import functools
import math

import jax
import jax.numpy as jnp
from jax import lax
from jax.experimental import pallas as pl
from jax.experimental.pallas import tpu as pltpu
from jax.sharding import PartitionSpec as P


WIDTH = 4
TIME_STEP = 0.25
PAD = 16
EDGE = WIDTH
LANES = 128

VMEM = pl.BlockSpec(memory_space=pltpu.VMEM)
SMEM = pl.BlockSpec(memory_space=pltpu.SMEM)
DEPTHS = (WIDTH, WIDTH - 1, WIDTH - 1, WIDTH - 1, WIDTH - 1)


def call(kernel, outs, args, scratch=(), scalars=0):
    need = sum(4 * math.prod(shape) for shape in list(outs) + list(scratch))
    need += sum(4 * math.prod(arg.shape) for arg in args[scalars:])
    return pl.pallas_call(
        kernel,
        out_shape=[jax.ShapeDtypeStruct(shape, jnp.float32) for shape in outs],
        in_specs=[SMEM] * scalars + [VMEM] * (len(args) - scalars),
        out_specs=[VMEM] * len(outs),
        scratch_shapes=[pltpu.VMEM(shape, jnp.float32) for shape in scratch],
        compiler_params=pltpu.CompilerParams(vmem_limit_bytes=need + 4 * 2**20),
    )(*args)


def first_faces(odd_ref, field, speed, signs, diffusivity, to_odd, to_slide, to_even, f, s, g, d, sems):
    nx = field.shape[0]
    copies = []
    for side in range(2):
        deep, short = (pl.ds(nx - n if side else 0, n) for n in DEPTHS[:2])
        for src, dst in (
            (field.at[deep], f.at[side]),
            (diffusivity.at[short], d.at[side]),
            (speed.at[:, short], s.at[side]),
            (signs.at[:, short], g.at[side]),
        ):
            copies.append(pltpu.make_async_copy(src, dst, sems.at[len(copies)]))
    for copy in copies:
        copy.start()
    for copy in copies:
        copy.wait()
    odd = odd_ref[0]
    for out, side in ((to_odd, odd), (to_even, 1 - odd)):
        for i in range(WIDTH):
            out[i] = f[side, i]
        for i in range(WIDTH - 1):
            out[WIDTH + i] = TIME_STEP * d[side, i]
            for k in range(3):
                scaled = TIME_STEP * s[side, k, i]
                out[WIDTH + (1 + k) * (WIDTH - 1) + i] = jnp.where(g[side, k, i] > 0, scaled, -scaled)
    for i in range(to_odd.shape[0]):
        to_slide[i] = to_odd[i]


def prepare(field, speed, signs, diffusivity, own, y_up, y_down, z_up, z_down):
    nx, rows = field.shape[:2]

    def plane(x, carry):
        own[x] = field[x]
        own[nx + x] = TIME_STEP * diffusivity[x]
        for d in range(3):
            scaled = TIME_STEP * speed[d, x]
            own[(2 + d) * nx + x] = jnp.where(signs[d, x] > 0, scaled, -scaled)
        return carry

    lax.fori_loop(0, nx, plane, 0)

    def edge(p, carry):
        y_up[p] = own[p, rows - WIDTH : rows, :]
        y_down[p] = own[p, 0:WIDTH, :]
        return carry

    lax.fori_loop(0, own.shape[0], edge, 0)

    def quantity(q, carry):
        for row in range(0, rows, 32):
            planes = [(WIDTH + i, own[q * nx + i, row : row + 32]) for i in range(nx)]
            up, down = pack_lanes(planes, 32)
            z_up[q, row : row + 32] = up
            z_down[q, row : row + 32] = down
        return carry

    lax.fori_loop(0, z_up.shape[0], quantity, 0)


def pack_lanes(planes, count):
    lane = lax.broadcasted_iota(jnp.int32, (count, LANES), 1)
    pair, lower = lane // (2 * WIDTH), lane % (2 * WIDTH) < WIDTH
    sums = [jnp.zeros((count, LANES), jnp.float32)] * 2
    for x, value in planes:
        m, k = x // 2, x % 2
        moved = pltpu.roll(value, (2 * WIDTH * m + WIDTH) % LANES, 1)
        sums[k] = jnp.where(pair == m, moved, sums[k])
    up = jnp.where(lower, sums[0], pltpu.roll(sums[1], WIDTH, 1))
    down = jnp.where(lower, pltpu.roll(sums[0], LANES - WIDTH, 1), sums[1])
    return up, down


def faces(odd, own, to_odd, to_slide, to_even, nx):
    a = jnp.where(odd > 0, nx - WIDTH, 0)
    b = jnp.where(odd > 0, 0, nx - WIDTH)
    for i in range(WIDTH):
        to_odd[i] = own[a + i]
        to_slide[i] = own[a + i]
        to_even[i] = own[b + i]


def pack_y(reach, place, *refs):
    *own, one, slid, three, up, down, held = refs
    crossed = place[1]
    rows, total = one.shape[1], one.shape[0]

    def wide(src):
        for i in range(total):
            up[reach * i : reach * (i + 1)] = src[i, rows - reach : rows, :]
            down[reach * i : reach * (i + 1)] = src[i, 0:reach, :]

    @pl.when(crossed > 0)
    def _():
        wide(slid)
        for i in range(total):
            held[i] = slid[i]

    @pl.when(crossed == 0)
    def _():
        wide(one)

    at = reach * total
    for src in (three, *own):
        for i in range(src.shape[0]):
            up[at : at + WIDTH] = src[i, rows - WIDTH : rows, :]
            down[at : at + WIDTH] = src[i, 0:WIDTH, :]
            at += WIDTH


def planes_of(q, nx, depths, own, sides):
    depth, at, total = depths[q], sum(depths[:q]), sum(depths)
    low = [(WIDTH - depth + i, sides, at + i, None) for i in range(depth)]
    mid = [(WIDTH + i, own, q * nx + i, q * nx + i) for i in range(nx)]
    high = [(WIDTH + nx + i, sides, total + at + i, None) for i in range(depth)]
    return low + mid + high


def fetch(src, out, sem):
    copy = pltpu.make_async_copy(src, out, sem)
    copy.start()
    copy.wait()


def place_sides(reach, place, one, slid, three, ylo, yhi, sides, joined):
    rows, total = one.shape[1], one.shape[0]
    odd, crossed, start = place[0], place[1], place[2]

    def framed(src, base, i, below, above):
        at = base * total + i
        sides[at, EDGE : EDGE + rows] = src[i]
        sides[at, EDGE - WIDTH : EDGE] = ylo[below : below + WIDTH]
        sides[at, EDGE + rows : EDGE + rows + WIDTH] = yhi[above : above + WIDTH]

    for i in range(total):
        framed(three, 1 - odd, i, reach * total + WIDTH * i, reach * total + WIDTH * i)

    @pl.when(crossed > 0)
    def _():
        for i in range(total):
            joined[i, 0:reach] = ylo[reach * i : reach * (i + 1)]
            joined[i, reach : reach + rows] = slid[i]
            joined[i, reach + rows :] = yhi[reach * i : reach * (i + 1)]
        for i in range(total):
            sides[odd * total + i, EDGE - WIDTH : EDGE + rows + WIDTH] = joined[i, pl.ds(start, rows + 2 * WIDTH)]

    @pl.when(crossed == 0)
    def _():
        for i in range(total):
            framed(one, odd, i, reach * (i + 1) - WIDTH, reach * i)


def pack_own_rims(ylo, yhi, z_up, z_down, up, down, low, high):
    rows = z_up.shape[1]
    nx = ylo.shape[0] // z_up.shape[0]
    for q in range(z_up.shape[0]):
        for row, rim in ((EDGE - WIDTH, ylo), (EDGE + rows, yhi)):
            last, first = pack_lanes([(WIDTH + i, rim[q * nx + i]) for i in range(nx)], WIDTH)
            up[q, row : row + WIDTH] = last
            down[q, row : row + WIDTH] = first
        up[q, EDGE : EDGE + rows] = z_up[q]
        down[q, EDGE : EDGE + rows] = z_down[q]

    def rim(p, carry):
        low[p] = ylo[p]
        high[p] = yhi[p]
        return carry

    lax.fori_loop(0, ylo.shape[0], rim, 0)


def side_slots(depths):
    return [(2 * sum(depths[:q]), depth) for q, depth in enumerate(depths)]


def pack_sides(depths, reach, place, *refs):
    one, slid, three, ylo, yhi, sides, up, down, joined = refs
    place_sides(reach, place, one, slid, three, ylo, yhi, sides, joined)
    total = one.shape[0]
    rows = up.shape[0] // 3
    for row in range(0, up.shape[0], rows):
        values = []
        for q, (slot, depth) in enumerate(side_slots(depths)):
            for i in range(depth):
                at = sum(depths[:q]) + i
                values.append((slot + i, sides[at, row : row + rows]))
                values.append((slot + depth + i, sides[total + at, row : row + rows]))
        up[row : row + rows], down[row : row + rows] = pack_lanes(values, rows)


def pack_z(depths, nx, reach, place, *refs):
    own, one, slid, three, ylo, yhi, sides, up, down, joined = refs
    place_sides(reach, place, one, slid, three, ylo, yhi, sides, joined)
    rows, total = one.shape[1], one.shape[0]
    later = WIDTH * total + reach * total
    for q in range(len(depths)):
        planes = planes_of(q, nx, depths, own, sides)
        for row, count in [(EDGE + r, 32) for r in range(0, rows, 32)] + [(EDGE - WIDTH, WIDTH), (EDGE + rows, WIDTH)]:
            values = []
            for x, src, index, p in planes:
                if p is None:
                    values.append((x, src[index, row : row + count]))
                elif count == WIDTH:
                    values.append((x, (ylo if row < EDGE else yhi)[later + WIDTH * p : later + WIDTH * (p + 1)]))
                else:
                    values.append((x, src[index, row - EDGE : row - EDGE + count]))
            up[q, row : row + count], down[q, row : row + count] = pack_lanes(values, count)


def derive(read, write):
    d = read(1)
    v = [read(2 + k) for k in range(3)]
    write(0, 1.0 - 6.0 * d - (v[0] + v[1] + v[2]))
    for k in range(3):
        write(1 + 2 * k, d + jnp.maximum(v[k], 0.0))
        write(2 + 2 * k, d + jnp.minimum(v[k], 0.0))


def advance(second, *refs):
    odd_ref, own = refs[0], refs[1]
    halo = refs[2:9]
    refs = refs[9:]
    if second:
        field_own, field_halo, depths = refs[0], refs[1:6], (WIDTH,)
        out = refs[6]
        refs = refs[7:]
    else:
        field_own, field_halo, depths = own, halo, DEPTHS
        out, to_odd, to_slide, to_even = refs[:4]
        refs = refs[4:]
    nx = out.shape[0]
    cells, coef, strip, strip_coef = refs
    rows = own.shape[1]
    high = rows + 2 * EDGE
    shift = PAD - EDGE

    for x, src, index, p in planes_of(0, nx, depths, field_own, field_halo[0]):
        if p is None:
            cells[0, x, shift : shift + high] = src[index]
            continue
        cells[0, x, PAD : PAD + rows] = src[index]
        at = field_halo[1].shape[0] - WIDTH * (nx - p)
        rim = (slice(at, at + WIDTH),) if second else (p,)
        cells[0, x, PAD - WIDTH : PAD] = field_halo[1][rim]
        cells[0, x, PAD + rows : PAD + rows + WIDTH] = field_halo[2][rim]
    lane = lax.broadcasted_iota(jnp.int32, (high, LANES), 1)
    inside = (lane >= WIDTH * WIDTH) & (lane < WIDTH * (WIDTH + nx))
    slots = side_slots(DEPTHS)

    def z_halo(q, side):
        slot, depth = slots[q]
        packed = halo[5 + side][...]
        low = pltpu.roll(packed, WIDTH * (WIDTH - depth - slot) % LANES, 1)
        top = pltpu.roll(packed, WIDTH * (WIDTH + nx - slot - depth) % LANES, 1)
        return jnp.where(inside, halo[3 + side][q], jnp.where(lane < WIDTH * WIDTH, low, top))

    for side in range(2):
        strip[0, side, shift : shift + high] = field_halo[3 + side][0] if second else z_halo(0, side)

        def write(k, value, side=side):
            strip_coef[k, side] = value

        derive(functools.partial(z_halo, side=side), write)
    for four in zip(*[planes_of(q, nx, DEPTHS, own, halo[0]) for q in range(1, 5)]):
        x, p = four[0][0], four[0][3]

        def at(row, count, x=x):
            def write(k, value):
                coef[k, x, row : row + count] = value

            return write

        offset = 0 if p is None else EDGE
        size = high // 3 if p is None else 16
        for r in range(0, high if p is None else rows, size):
            derive(lambda q, r=r, n=size, four=four: four[q - 1][1][four[q - 1][2], r : r + n], at(offset + r, size))
        if p is not None:
            derive(lambda q, four=four: halo[1][four[q - 1][3]], at(EDGE - WIDTH, WIDTH))
            derive(lambda q, four=four: halo[2][four[q - 1][3]], at(EDGE + rows, WIDTH))

    for step in range(1, WIDTH + 1):
        src, dst = (step - 1) % 2, step % 2
        last = step == WIDTH
        for row, size in ((EDGE, rows),) if last else ((0, high),):
            here = shift + row
            lane = lax.broadcasted_iota(jnp.int32, (size, LANES), 1)
            start, end = lane == 0, lane == LANES - 1
            group, place = lane // WIDTH, lane % WIDTH
            low, top = (strip[src, side, here : here + size] for side in range(2))
            beyond = jnp.where(place == WIDTH - 1, low, pltpu.roll(top, WIDTH - 2, 1))
            inner = jnp.zeros((size, LANES), jnp.float32)
            before = cells[src, step - 1, here : here + size]
            mid = cells[src, step, here : here + size]
            for x in range(step, nx + 2 * WIDTH - step):
                after = cells[src, x + 1, here : here + size]
                turn = WIDTH * x + WIDTH - 1
                outer = pltpu.roll(beyond, (LANES - turn) % LANES, 1)
                if not last:
                    inner = jnp.where(group == x, pltpu.roll(mid, turn % LANES, 1), inner)
                c = [coef[k, x, row : row + size] for k in range(7)]
                new = c[0] * mid + c[1] * before + c[2] * after
                new += c[3] * cells[src, x, here - 1 : here - 1 + size]
                new += c[4] * cells[src, x, here + 1 : here + 1 + size]
                new += c[5] * jnp.where(start, outer, pltpu.roll(mid, 1, 1))
                new += c[6] * jnp.where(end, outer, pltpu.roll(mid, LANES - 1, 1))
                if last:
                    out[x - WIDTH, row - EDGE : row - EDGE + size] = new
                else:
                    cells[dst, x, here : here + size] = new
                before, mid = mid, after
            if last:
                continue
            for side in range(2):
                mid = low if side == 0 else top
                below, above = pltpu.roll(mid, 1, 1), pltpu.roll(mid, LANES - 1, 1)
                if side == 0:
                    above = jnp.where(place == WIDTH - 1, inner, above)
                else:
                    below = jnp.where(place == 0, pltpu.roll(inner, LANES - (WIDTH - 2), 1), below)
                c = [strip_coef[k, side, row : row + size] for k in range(7)]
                new = c[0] * mid + c[1] * pltpu.roll(mid, WIDTH, 1) + c[2] * pltpu.roll(mid, LANES - WIDTH, 1)
                new += c[3] * strip[src, side, here - 1 : here - 1 + size]
                new += c[4] * strip[src, side, here + 1 : here + 1 + size]
                new += c[5] * below + c[6] * above
                strip[dst, side, here : here + size] = new
    if not second:
        faces(odd_ref[0], out, to_odd, to_slide, to_even, nx)


def exchange_x(to_odd, to_slide, to_even, shift, beside, args):
    count_x, count_y = lax.axis_size("gx"), lax.axis_size("gy")
    even = [(i, i + 1) for i in range(0, count_x, 2)]
    odd = [(i * count_y + j, (i + 1) * count_y + j) for i in range(1, count_x - 1, 2) for j in range(count_y)]
    if to_odd.shape[0] > WIDTH:
        odd += [(i * count_y + j, i * count_y + j + 1) for i in (0, count_x - 1) for j in range(0, count_y, 2)]

    def slide(k):
        pairs = []
        for j in range(count_y):
            top = (count_x - 1) * count_y + (j + k) % count_y
            pairs += [(j, top), (top, j)]
        return lambda a, *rest: (lax.ppermute(a, ("gx", "gy"), pairs), *beside(*rest))

    three = lax.ppermute(to_even, "gx", even + [(b, a) for a, b in even])
    one = lax.ppermute(to_odd, ("gx", "gy"), odd + [(b, a) for a, b in odd])
    slid, *rest = lax.switch(shift, [slide(k) for k in range(count_y)], to_slide, *args)
    return one, slid, three, rest


def shift_both(axis, up, down):
    n = lax.axis_size(axis)
    forth = [(i, (i + 1) % n) for i in range(n)]
    return lax.ppermute(up, axis, forth), lax.ppermute(down, axis, [(b, a) for a, b in forth])


def first_halo(inputs, to_odd, to_slide, to_even, shift, place):
    total, rows, _ = to_odd.shape
    nx, count = inputs[0].shape[0], len(DEPTHS)
    high = rows + 2 * EDGE
    reach = rows // 2 + WIDTH

    def beside(*inputs):
        rim, lanes = (count * nx, WIDTH, LANES), (count, rows, LANES)
        own, up, down, z_up, z_down = call(prepare, [(count * nx, rows, LANES), rim, rim, lanes, lanes], inputs)
        return own, *shift_both("gy", up, down), z_up, z_down

    one, slid, three, (own, y_low, y_high, z_up, z_down) = exchange_x(to_odd, to_slide, to_even, shift, beside, inputs)
    shape = (reach * total + WIDTH * total, LANES)
    up, down, slid = call(functools.partial(pack_y, reach), [shape] * 2 + [slid.shape], [place, one, slid, three], (), 1)
    up, down, z_up, z_down = lax.optimization_barrier((up, down, z_up, z_down))
    ylo, yhi = shift_both("gy", up, down)
    shapes = [(count, high, LANES)] * 2 + [y_low.shape] * 2
    z_up, z_down, y_low, y_high = call(pack_own_rims, shapes, [y_low, y_high, z_up, z_down])
    z_low, z_high = shift_both("gz", z_up, z_down)
    sides, up, down = call(
        functools.partial(pack_sides, DEPTHS, reach),
        [(2 * total, high, LANES), (high, LANES), (high, LANES)],
        [place, one, slid, three, ylo, yhi],
        [(total, rows + 2 * reach, LANES)],
        1,
    )
    return own, [sides, y_low, y_high, z_low, z_high, *shift_both("gz", up, down)]


def second_halo(field, own, to_odd, to_slide, to_even, shift, place):
    total, rows, _ = to_odd.shape
    nx = field.shape[0]
    reach = rows // 2 + WIDTH
    high = rows + 2 * EDGE
    one, slid, three, _ = exchange_x(to_odd, to_slide, to_even, shift, lambda: (), [])
    shape = (reach * total + WIDTH * total + WIDTH * nx, LANES)
    args = [place, field, one, slid, three]
    up, down, slid = call(functools.partial(pack_y, reach), [shape] * 2 + [slid.shape], args, (), 1)
    up, down, own = lax.optimization_barrier((up, down, own))
    ylo, yhi = shift_both("gy", up, down)
    own = pl.pallas_call(
        fetch,
        out_shape=jax.ShapeDtypeStruct(own.shape, own.dtype),
        in_specs=[pl.BlockSpec(memory_space=pl.ANY)],
        out_specs=VMEM,
        scratch_shapes=[pltpu.SemaphoreType.DMA(())],
        compiler_params=pltpu.CompilerParams(vmem_limit_bytes=4 * 2**20),
    )(own)
    shape = (1, high, LANES)
    sides, up, down = call(
        functools.partial(pack_z, (WIDTH,), nx, reach),
        [(2 * total, high, LANES), shape, shape],
        [place, field, one, slid, three, ylo, yhi],
        [(total, rows + 2 * reach, LANES)],
        1,
    )
    return own, [sides, ylo, yhi, *shift_both("gz", up, down)]


def body(concentration, speed, signs, diffusivity, shear):
    nx, rows, lanes = concentration.shape
    count_x, count_y = lax.axis_size("gx"), lax.axis_size("gy")
    x_index = lax.axis_index("gx")
    blocks = (shear[0] + rows // 2) // rows
    shift, rest = blocks % count_y, shear[0] - blocks * rows
    crossed = (x_index == 0) | (x_index == count_x - 1)
    start = rows // 2 + jnp.where(x_index == 0, rest, -rest)
    odd = (x_index % 2).astype(jnp.int32).reshape(1)
    place = jnp.stack([x_index % 2, crossed.astype(jnp.int32), jnp.where(crossed, start, 0)]).astype(jnp.int32)
    face = (sum(DEPTHS), rows, lanes)
    inputs = [concentration, speed, signs, diffusivity]
    short = (2, WIDTH - 1, rows, lanes)
    to_odd, to_slide, to_even = pl.pallas_call(
        first_faces,
        out_shape=[jax.ShapeDtypeStruct(face, jnp.float32)] * 3,
        in_specs=[SMEM] + [pl.BlockSpec(memory_space=pl.ANY)] * 4,
        out_specs=[VMEM] * 3,
        scratch_shapes=[
            pltpu.VMEM((2, WIDTH, rows, lanes), jnp.float32),
            pltpu.VMEM((2, 3, *short[1:]), jnp.float32),
            pltpu.VMEM((2, 3, *short[1:]), jnp.int32),
            pltpu.VMEM(short, jnp.float32),
            pltpu.SemaphoreType.DMA((8,)),
        ],
        compiler_params=pltpu.CompilerParams(vmem_limit_bytes=8 * 2**20),
    )(odd, *inputs)
    own, halo = first_halo(inputs, to_odd, to_slide, to_even, shift, place)
    high = rows + 2 * EDGE
    wide = nx + 2 * WIDTH
    scratch = [(2, wide, rows + 2 * PAD, lanes), (7, wide, high, lanes), (2, 2, rows + 2 * PAD, lanes), (7, 2, high, lanes)]
    face = (WIDTH, rows, lanes)
    field, to_odd, to_slide, to_even = call(
        functools.partial(advance, False), [(nx, rows, lanes), face, face, face], [odd, own, *halo], scratch, 1
    )
    own, later = second_halo(field, own, to_odd, to_slide, to_even, shift, place)
    (field,) = call(
        functools.partial(advance, True), [(nx, rows, lanes)], [odd, own, *halo, field, *later], scratch, 1
    )
    return field


def solution(mesh):
    placed = (
        P("gx", "gy", "gz"),
        P(None, "gx", "gy", "gz"),
        P(None, "gx", "gy", "gz"),
        P("gx", "gy", "gz"),
        P(),
    )

    return jax.shard_map(body, mesh=mesh, in_specs=placed, out_specs=P("gx", "gy", "gz"), check_vma=False)
```
